32 devices in a mesh: dp: 8 (over z, x), mp: 4 (over y, core).
Axes of the slice: x: 2, y: 2, z: 4, core: 2. Of those that a mesh axis runs over, the one named last changes fastest.
Arguments:
- hidden: bfloat16 [8, 512, 4608], P('dp', 'mp'), may hold values from -6 to 6
- lengths: int32 [8], P('dp'), may hold values from 64 to 512
- norm_gain: float32 [4608], replicated, may hold values from 0.25 to 1.75
- w_query: bfloat16 [4608, 2048], P('dp', 'mp'), may hold values from -0.09375 to 0.09375
- w_key: bfloat16 [4608, 1024], P('dp', 'mp'), may hold values from -0.09375 to 0.09375
- w_value: bfloat16 [4608, 1024], P('dp', 'mp'), may hold values from -0.09375 to 0.09375
- w_out: bfloat16 [2048, 4608], P('mp', 'dp'), may hold values from -0.125 to 0.125
- post_gain: float32 [4608], replicated, may hold values from 0.25 to 1.75
Outputs:
- mixed: bfloat16 [8, 512, 4608], P('dp', 'mp')
- key_cache: bfloat16 [8, 512, 1024], P('dp', None, 'mp')
- value_cache: bfloat16 [8, 512, 1024], P('dp', None, 'mp')
The draws below stay inside these ranges and needn't reach their ends.
All inputs are finite; a program needn't handle non-finite values.
Results may differ from the reference program's by a relative error of at most 0.01.
Values may be sent and summed in bfloat16 or wider, within the bound.
A program may use at most 128 MiB of HBM per device.

```python
import jax
import jax.numpy as jnp
from jax import lax

D = 4608
HD = 128
QH = 16
KVH = 8
MAXLEN = 512
MINLEN = 64
ROLLOUTS = 8
N_MP = 4


def place_ends(values, key, low, largest):
    spot = [jax.random.randint(jax.random.fold_in(key, axis), (), 0, length) for axis, length in enumerate(values.shape)]
    widest = values.shape.index(max(values.shape))
    beside = spot[:widest] + [(spot[widest] + 1) % values.shape[widest]] + spot[widest + 1:]
    return values.at[tuple(spot)].set(low).at[tuple(beside)].set(largest)


def block_levels(own_key, shape, pieces, least, largest):
    level, own = 1.0, jax.random.fold_in(own_key, 6)
    for position, shards_of in pieces:
        steps = jnp.exp(jax.random.uniform(jax.random.fold_in(own, position), (shards_of,), jnp.float32, least / len(pieces), largest / len(pieces)))
        level = level * jnp.repeat(steps, shape[position] // shards_of).reshape([-1 if axis == position else 1 for axis in range(len(shape))])
    return level


def centred(stream_key, shape, scale, limit, cuts=(), kind=jnp.bfloat16):
    result = scale * jax.random.normal(stream_key, shape, jnp.float32)
    if cuts:
        result = result * block_levels(stream_key, shape, cuts, -0.22, 0.18)
    return jnp.clip(result, -limit, limit).astype(kind)


def setup_inputs(seed: int = 0) -> dict:
    seeds = jax.random.split(jax.random.key(seed), 9)
    hidden = centred(seeds[0], (ROLLOUTS, MAXLEN, D), 1.0, 6.0, ((0, 8), (1, 4)))
    lengths = place_ends(jax.random.randint(seeds[1], (ROLLOUTS,), MINLEN, MAXLEN + 1), jax.random.fold_in(seeds[1], 1), MINLEN, MAXLEN).astype(jnp.int32)
    norm_gain = jnp.clip(1.0 + 0.15 * jax.random.normal(seeds[2], (D,), jnp.float32), 0.25, 1.75)
    w_query = centred(seeds[3], (D, QH * HD), D ** -0.5, 0.09375, ((0, 8), (1, 4)))
    w_key = centred(seeds[4], (D, KVH * HD), D ** -0.5, 0.09375, ((0, 8), (1, 4)))
    w_value = centred(seeds[5], (D, KVH * HD), D ** -0.5, 0.09375, ((0, 8), (1, 4)))
    w_out = centred(seeds[6], (QH * HD, D), (QH * HD) ** -0.5, 0.125, ((0, 4), (1, 8)))
    post_gain = jnp.clip(1.0 + 0.15 * jax.random.normal(seeds[7], (D,), jnp.float32), 0.25, 1.75)
    return {"hidden": hidden, "lengths": lengths, "norm_gain": norm_gain, "w_query": w_query, "w_key": w_key, "w_value": w_value, "w_out": w_out, "post_gain": post_gain}


def rotate(values, positions):
    half = values.shape[-1] // 2
    freqs = 10000.0 ** (-jnp.arange(half, dtype=jnp.float32) / half)
    angles = positions.astype(jnp.float32)[:, None] * freqs[None, :]
    cosine = jnp.cos(angles)[:, None, :]
    sine = jnp.sin(angles)[:, None, :]
    first = values[..., :half]
    second = values[..., half:]
    return jnp.concatenate([first * cosine - second * sine, second * cosine + first * sine], axis=-1)

def one_rollout(args, norm_gain, w_query, w_key, w_value, w_out, post_gain):
    rows, length = args
    maxlen = rows.shape[0]
    group = QH // KVH
    rows_f = rows.astype(jnp.float32)
    normed = (rows_f * lax.rsqrt(lax.optimization_barrier(jnp.mean(rows_f * rows_f, axis=-1, keepdims=True)) + 1e-06) * norm_gain).astype(jnp.bfloat16)
    positions = jnp.arange(maxlen, dtype=jnp.int32)
    qraw = jnp.dot(normed, w_query, preferred_element_type=jnp.float32).reshape(maxlen, QH, HD)
    kraw = jnp.dot(normed, w_key, preferred_element_type=jnp.float32).reshape(maxlen, KVH, HD)
    vraw = jnp.dot(normed, w_value, preferred_element_type=jnp.float32).reshape(maxlen, KVH, HD)
    query = (rotate(qraw, positions) * 144.0 ** (-0.5)).astype(jnp.bfloat16)
    key = rotate(kraw, positions).astype(jnp.bfloat16)
    value = vraw.astype(jnp.bfloat16)
    grouped = query.reshape(maxlen, KVH, group, HD).astype(jnp.float32)
    score = jnp.einsum('qkgd,tkd->kgqt', grouped, key.astype(jnp.float32))
    score = 50.0 * jnp.tanh(score / 50.0)
    keep = (positions[None, :] <= positions[:, None]) & (positions[None, :] < length)
    score = jnp.where(keep[None, None], score, -1e+30)
    top = lax.optimization_barrier(jnp.max(score, axis=-1, keepdims=True))
    expo = jnp.exp(score - top)
    weights = (expo / lax.optimization_barrier(jnp.sum(expo, axis=-1, keepdims=True))).astype(jnp.bfloat16)
    attended = jnp.einsum('kgqt,tkd->qkgd', weights.astype(jnp.float32), value.astype(jnp.float32))
    attended = attended.reshape(maxlen, QH * HD).astype(jnp.bfloat16)
    cols = QH * HD // N_MP
    projected = jnp.zeros((maxlen, D), jnp.float32)
    for part in range(N_MP):
        partial_value = jnp.dot(attended[:, part * cols:(part + 1) * cols], w_out[part * cols:(part + 1) * cols], preferred_element_type=jnp.float32)
        projected = projected + partial_value.astype(jnp.bfloat16).astype(jnp.float32)
    post = projected * lax.rsqrt(lax.optimization_barrier(jnp.mean(projected * projected, axis=-1, keepdims=True)) + 1e-06) * post_gain
    live = (positions < length)[:, None]
    mixed = jnp.where(live, rows_f + post, 0.0).astype(jnp.bfloat16)
    key_rows = jnp.where(live, key.reshape(maxlen, KVH * HD), jnp.zeros((), jnp.bfloat16))
    value_rows = jnp.where(live, value.reshape(maxlen, KVH * HD), jnp.zeros((), jnp.bfloat16))
    return (mixed, key_rows, value_rows)

def reference(hidden, lengths, norm_gain, w_query, w_key, w_value, w_out, post_gain):

    def step(args):
        return one_rollout(args, norm_gain, w_query, w_key, w_value, w_out, post_gain)
    mixed, key_cache, value_cache = lax.map(step, (hidden, lengths))
    return (mixed, key_cache, value_cache)
```

```python
import functools

import jax
import jax.numpy as jnp
import numpy as np
from jax import lax
from jax.experimental import pallas as pl
from jax.experimental.pallas import tpu as pltpu
from jax.sharding import PartitionSpec as P

HD = 128
LANES = 128
MESH = pl.DeviceIdType.MESH
UP, DOWN = 0, 1
OWN, OTHER = 0, 1


def tables(maxlen):
    half = HD // 2
    freqs = 10000.0 ** (-np.arange(half, dtype=np.float64) / half)
    angles = np.arange(maxlen, dtype=np.float64)[:, None] * freqs[None, :]
    cosine, sine = np.cos(angles), np.sin(angles)
    return (
        np.concatenate([cosine, cosine], axis=1).astype(np.float32),
        np.concatenate([-sine, sine], axis=1).astype(np.float32),
    )


def cut(rows):
    pieces, start = [], 0
    while start < rows:
        size = min(256, rows - start)
        pieces.append((start, size))
        start += size
    return pieces


def kernel(
    n_dp, n_mp, pieces,
    len_ref, hid_in, ngain_in, wq, wk, wv, wo, pgain_in, cos_in, sin_in,
    mixed, key_out, val_out,
    *scratch,
):
    ns = len(pieces)
    (
        hid, ngain_t, pgain_t, ngain, pgain, cos_ref, sin_ref,
        wbuf, obuf, nbuf, acc, pout, pin, kbuf, vbuf, vext, att, sq, mbuf,
    ) = scratch[:19]
    rest = scratch[19:]
    psend, inbox, precv, xout, yall = (rest[i * ns : (i + 1) * ns] for i in range(5))
    (
        load_sem, zsend, zrecv, xsend, xmate, xfar, xrecv, qsend, qrecv, asend, arecv,
        hsend, hrecv, fsend, frecv, csend, crecv, osem,
    ) = rest[5 * ns :]

    nz = n_dp // 2
    pairs = n_mp // 2
    me, mp = lax.axis_index("dp"), lax.axis_index("mp")
    z, x = me // 2, me % 2
    side, slot = mp % 2, mp // 2
    partner = me + 1 - 2 * x
    mate = mp + 1 - 2 * side
    local_len, width = hid.shape
    maxlen = local_len * n_mp
    fcols = width // n_dp
    qw, kw = wq.shape[1], wk.shape[1]
    nq = qw // kw
    nc = 2 + nq
    q_heads, kv_heads = qw // HD, kw // HD
    can_up, can_down = z < nz - 1, z > 0
    middle = can_up & can_down
    f32, bf16 = jnp.float32, jnp.bfloat16

    def remote(src, dst, send, recv, dp_index, mp_index):
        return pltpu.make_async_remote_copy(
            src_ref=src, dst_ref=dst, send_sem=send, recv_sem=recv,
            device_id=(dp_index, mp_index), device_id_type=MESH,
        )

    load_w = [
        pltpu.make_async_copy(wk, wbuf.at[z, 0], load_sem.at[0]),
        pltpu.make_async_copy(wv, wbuf.at[z, 1], load_sem.at[1]),
    ] + [
        pltpu.make_async_copy(wq.at[:, pl.ds(j * kw, kw)], wbuf.at[z, 2 + j], load_sem.at[2 + j])
        for j in range(nq)
    ]
    load_o = pltpu.make_async_copy(wo, obuf.at[z], load_sem.at[nc])
    load_x = [
        pltpu.make_async_copy(hid_in, hid, load_sem.at[nc + 1]),
        pltpu.make_async_copy(ngain_in, ngain_t, load_sem.at[nc + 2]),
    ]
    load_r = [
        pltpu.make_async_copy(pgain_in, pgain_t, load_sem.at[nc + 3]),
        pltpu.make_async_copy(cos_in, cos_ref, load_sem.at[nc + 4]),
        pltpu.make_async_copy(sin_in, sin_ref, load_sem.at[nc + 5]),
    ]
    for load in load_w[:1] + load_x + load_w[1:] + [load_o] + load_r:
        load.start()

    barrier = pltpu.get_barrier_semaphore()

    def greet(dp_index, mp_index):
        pl.semaphore_signal(barrier, inc=1, device_id=(dp_index, mp_index), device_id_type=MESH)

    greet(partner, mp)
    for step in range(1, n_mp):
        greet(me, lax.rem(mp + step, n_mp))

    @pl.when(can_up)
    def _():
        greet(me + 2, mp)

    @pl.when(can_down)
    def _():
        greet(me - 2, mp)

    pl.semaphore_wait(
        barrier, n_mp + jnp.where(can_up, 1, 0) + jnp.where(can_down, 1, 0)
    )

    def item(c, origin):
        if c < nc:
            return wbuf.at[origin, c]
        start, size = pieces[c - nc]
        return obuf.at[origin, pl.ds(start, size)]

    def copy(c, origin, way):
        ref = item(c, origin)
        return remote(
            ref, ref, zsend.at[c, way, origin], zrecv.at[c, origin],
            (me + 2, me - 2)[way], mp,
        )

    def send_own(c):
        @pl.when(can_up)
        def _():
            copy(c, z, UP).start()

        @pl.when(can_down)
        def _():
            copy(c, z, DOWN).start()

    def relay(c, k):
        below, above = z - k, z + k

        @pl.when(below >= 0)
        def _():
            copy(c, below, UP).wait_recv()

            @pl.when(can_up)
            def _():
                copy(c, below, UP).start()

        @pl.when(above < nz)
        def _():
            copy(c, above, DOWN).wait_recv()

            @pl.when(can_down)
            def _():
                copy(c, above, DOWN).start()

    def relays(c, first, last):
        def body(k, carry):
            relay(c, k)
            return carry

        lax.fori_loop(first, last, body, 0)

    def rows_of(parity, block):
        return pl.ds(pl.multiple_of(parity * maxlen + block * local_len, local_len), local_len)

    def region(parity, block):
        return nbuf.at[:, rows_of(parity, block), :]

    def across():
        return remote(
            nbuf.at[:, pl.ds(2 * maxlen, local_len), :], region(x, mp),
            xsend.at[0], xrecv.at[x, mp], partner, mp,
        )

    def to_mate(parity, block):
        return remote(
            region(parity, block), region(parity, block),
            xmate.at[parity, block // 2], xrecv.at[parity, block], me, mate,
        )

    def to_far(parity, step):
        return remote(
            region(parity, mp), region(parity, mp),
            xfar.at[parity, step - 1], xrecv.at[parity, mp], me, lax.rem(mp + 2 * step, n_mp),
        )

    def arrived(parity, block):
        return remote(
            region(parity, block), region(parity, block),
            xsend.at[0], xrecv.at[parity, block], me, mate,
        )

    def spread(parity):
        for step in range(1, pairs):
            to_far(parity, step).start()
        to_mate(parity, mp).start()

    def pass_on(parity):
        for step in range(1, pairs):
            block = lax.rem(mp + 2 * step, n_mp)
            arrived(parity, block).wait_recv()
            to_mate(parity, block).start()

    load_w[0].wait()
    send_own(0)
    for load in load_x:
        load.wait()
    for t in range(width // LANES):
        ngain[:, t * LANES : (t + 1) * LANES] = ngain_t[t : t + 1, :]
    total = jnp.zeros((local_len, LANES), f32)
    for t in range(width // LANES):
        rows = hid[:, t * LANES : (t + 1) * LANES].astype(f32)
        total = total + rows * rows
    scale = lax.rsqrt(jnp.sum(total, axis=-1, keepdims=True) / width + 1e-06)
    for block in range(n_dp):
        span = slice(block * fcols, (block + 1) * fcols)
        rows = hid[:, span].astype(f32)
        first = jnp.where(x == block % 2, x * maxlen + mp * local_len, 2 * maxlen)
        nbuf[block // 2, pl.ds(pl.multiple_of(first, local_len), local_len), :] = (
            rows * scale * ngain[:, span]
        ).astype(bf16)
    across().start()
    spread(x)
    for c in range(1, min(3, nc)):
        load_w[c].wait()
        send_own(c)
    acc[...] = jnp.zeros_like(acc)

    def rollout_rows(parity):
        return pl.ds(pl.multiple_of(parity * maxlen, maxlen), maxlen)

    def swap(c):
        return remote(pout.at[c], pin.at[c], qsend.at[c], qrecv.at[c], partner, mp)

    def compute(c):
        def half(parity):
            rows = rollout_rows(parity)

            def body(k, carry):
                acc[c, rows, :] += jnp.dot(
                    nbuf[k, rows, :], wbuf[k, c], preferred_element_type=f32
                )
                return carry

            lax.fori_loop(0, nz, body, 0)

        half(1 - x)
        pout[c] = acc[c, rollout_rows(1 - x), :].astype(bf16)
        swap(c).start()
        half(x)

    length = len_ref[0]
    live = lax.broadcasted_iota(jnp.int32, (maxlen, HD), 0) < length

    def rotated(block, span):
        return block * cos_ref[span, :] + pltpu.roll(block, HD // 2, 1) * sin_ref[span, :]

    everything = slice(0, maxlen)

    def keys_done():
        swap(0).wait_recv()
        for h in range(kv_heads):
            cols = slice(h * HD, (h + 1) * HD)
            raw = acc[0, rollout_rows(x), cols] + pin[0, :, cols].astype(f32)
            kbuf[:, cols] = jnp.where(live, rotated(raw, everything), 0.0).astype(bf16)

    def values_done():
        swap(1).wait_recv()
        for h in range(kv_heads):
            cols = slice(h * HD, (h + 1) * HD)
            raw = acc[1, rollout_rows(x), cols] + pin[1, :, cols].astype(f32)
            value = jnp.where(live, raw, 0.0).astype(bf16)
            vbuf[:, cols] = value
            vext[h, :, :HD] = value
            vext[h, :, HD:] = jnp.where(live, 1.0, 0.0).astype(bf16)

    def share(j, parity):
        ref = att.at[parity, :, pl.ds(j * kw, kw)]
        return remote(ref, ref, asend.at[j], arecv.at[j], partner, mp)

    def attend(j):
        swap(2 + j).wait_recv()
        for i in range(kv_heads):
            h = j * kv_heads + i
            kv = h * kv_heads // q_heads
            cols, kcols = slice(i * HD, (i + 1) * HD), slice(kv * HD, (kv + 1) * HD)
            for r in range(n_mp):
                span, seen = slice(r * local_len, (r + 1) * local_len), (r + 1) * local_len
                raw = acc[2 + j, rows_of(x, r), cols] + pin[2 + j, span, cols].astype(f32)
                query = (rotated(raw, span) * 144.0 ** (-0.5)).astype(bf16)
                score = lax.dot_general(
                    query, kbuf[:seen, kcols], (((1,), (1,)), ((), ())),
                    preferred_element_type=f32,
                )
                row = lax.broadcasted_iota(jnp.int32, score.shape, 0) + r * local_len
                col = lax.broadcasted_iota(jnp.int32, score.shape, 1)
                expo = jnp.exp2(jnp.tanh(score * (1.0 / 50.0)) * (50.0 * np.log2(np.e)))
                expo = jnp.where(col <= row, expo, 0.0).astype(bf16)
                both = jnp.dot(expo, vext[kv, :seen, :], preferred_element_type=f32)
                att[x, span, h * HD : (h + 1) * HD] = (both[:, :HD] / both[:, HD:]).astype(bf16)
        share(j, x).start()

    relays(0, 1, 2)
    arrived(1 - x, mp).wait_recv()
    spread(1 - x)
    pass_on(x)
    relays(0, 2, nz)
    pass_on(1 - x)
    for c in range(3, nc):
        load_w[c].wait()
        send_own(c)
    load_o.wait()

    @pl.when(jnp.logical_not(middle))
    def _():
        for s in range(ns):
            send_own(nc + s)

    for parity in (x, 1 - x):
        for step in range(pairs):
            arrived(parity, lax.rem(mate + 2 * step, n_mp)).wait_recv()
    compute(0)
    relays(1, 1, nz)
    compute(1)
    for load in load_r:
        load.wait()
    for t in range(width // LANES):
        pgain[:, t * LANES : (t + 1) * LANES] = pgain_t[t : t + 1, :]
    keys_done()
    for j in range(nq):
        c = 2 + j
        relays(c, 1, 2)
        if j == 0:
            relays(c, 2, nz)
            compute(c)
            values_done()
        else:
            attend(j - 1)
            relays(c, 2, nz)
            if j == nq - 1:
                @pl.when(middle)
                def _():
                    for s in range(ns):
                        send_own(nc + s)
            compute(c)
    if nq == 1:
        @pl.when(middle)
        def _():
            for s in range(ns):
                send_own(nc + s)

    out_k = pltpu.make_async_copy(kbuf, key_out, osem.at[0])
    out_v = pltpu.make_async_copy(vbuf, val_out, osem.at[1])
    out_k.start()
    out_v.start()

    def hand(s, zk, role, parity):
        return remote(
            psend[s].at[zk, parity, 1 - side], inbox[s].at[zk, parity],
            hsend.at[s, zk, role], hrecv.at[s, zk, role], me, mate,
        )

    def far(s, zk, role, parity, step):
        target = lax.rem(mp + 2 * step, n_mp)
        return remote(
            psend[s].at[zk, parity, side, target // 2], precv[s].at[zk, parity, step - 1],
            fsend.at[s, zk, role, step - 1], frecv.at[s, zk, role, step - 1], me, target,
        )

    def back(s, zk, parity):
        return remote(
            xout[s].at[zk], yall[s].at[parity, zk], csend.at[s, zk], crecv.at[s, zk], partner, mp
        )

    def parity_of(role):
        return x if role == OWN else 1 - x

    def produce(s, zk, role):
        start, size = pieces[s]
        parity = parity_of(role)
        part = lax.dot_general(
            att[parity], obuf[zk, start : start + size, :], (((1,), (1,)), ((), ())),
            preferred_element_type=f32,
        ).astype(bf16)
        for p in range(n_mp):
            psend[s][zk, parity, p % 2, p // 2] = part[p * local_len : (p + 1) * local_len]
        hand(s, zk, role, parity).start()

    def combine(s, zk, role):
        parity = parity_of(role)
        hand(s, zk, role, parity).wait_recv()
        for step in range(1, pairs):
            q = lax.rem(mp + 2 * step, n_mp) // 2
            both = psend[s][zk, parity, side, q].astype(f32) + inbox[s][zk, parity, q].astype(f32)
            psend[s][zk, parity, side, q] = both.astype(bf16)
            far(s, zk, role, parity, step).start()

    def measure(value):
        value = value.astype(f32)
        sq[...] += jnp.sum(value * value, axis=-1, keepdims=True)

    def settle(s, zk, role):
        parity = parity_of(role)
        value = psend[s][zk, parity, side, slot].astype(f32)
        value = value + inbox[s][zk, parity, slot].astype(f32)
        for step in range(1, pairs):
            far(s, zk, role, parity, step).wait_recv()
            value = value + precv[s][zk, parity, step - 1].astype(f32)
        value = value.astype(bf16)
        if role == OWN:
            yall[s][x, zk] = value
            measure(value)
        else:
            xout[s][zk] = value
            back(s, zk, x).start()

    def around(k, act):
        def body(way, carry):
            zk = z + k * (2 * way - 1)

            @pl.when((zk >= 0) & (zk < nz) & ((way == 0) | (k > 0)))
            def _():
                act(zk)

            return carry

        lax.fori_loop(0, 2, body, 0)

    def near(act):
        def body(k, carry):
            around(k, act)
            return carry

        lax.fori_loop(0, min(2, nz), body, 0)

    for s in range(ns):
        relays(nc + s, 1, min(2, nz))
    attend(nq - 1)
    sq[...] = jnp.zeros_like(sq)
    for role in (OWN, OTHER):
        if role == OTHER:
            for j in range(nq):
                share(j, 1 - x).wait_recv()
        for s in range(ns):
            near(functools.partial(produce, s, role=role))
        for s in range(ns):
            near(functools.partial(combine, s, role=role))

    def settle_near():
        for role in (OWN, OTHER):
            for s in range(ns):
                near(functools.partial(settle, s, role=role))

    def settle_at(k):
        for s in range(ns):
            def both(zk, s=s):
                for role in (OWN, OTHER):
                    settle(s, zk, role)

            around(k, both)

    def late(k, carry):
        for s in range(ns):
            if s == ns - 1:
                @pl.when(k == 2)
                def _():
                    settle_near()

                @pl.when(k > 2)
                def _():
                    settle_at(k - 1)

            relay(nc + s, k)

            def make(zk, s=s):
                for role in (OWN, OTHER):
                    produce(s, zk, role)

            def join(zk, s=s):
                for role in (OWN, OTHER):
                    combine(s, zk, role)

            around(k, make)
            around(k, join)
        return carry

    if nz > 2:
        lax.fori_loop(2, nz, late, 0)
        settle_at(nz - 1)
    else:
        settle_near()

    def collect(zk, carry):
        for s in range(ns):
            back(s, zk, 1 - x).wait_recv()
            measure(yall[s][1 - x, zk])
        return carry

    lax.fori_loop(0, nz, collect, 0)

    scale = lax.rsqrt(sq[...] / width + 1e-06)
    halves = 2
    tall = local_len // halves
    outs = []
    for part in range(halves):
        rows = slice(part * tall, (part + 1) * tall)
        for block in range(n_dp):
            for s, (start, size) in enumerate(pieces):
                span = slice(block * fcols + start, block * fcols + start + size)
                own = (
                    lax.broadcasted_iota(jnp.int32, (tall, size), 0) + mp * local_len + part * tall
                    < length
                )
                post = yall[s][block % 2, block // 2, rows, :].astype(f32)
                post = post * scale[rows] * pgain[:, span]
                mbuf[rows, span] = jnp.where(
                    own, hid[rows, span].astype(f32) + post, 0.0
                ).astype(bf16)
        out = pltpu.make_async_copy(
            mbuf.at[pl.ds(part * tall, tall)], mixed.at[pl.ds(part * tall, tall)],
            osem.at[2 + part],
        )
        out.start()
        outs.append(out)

    def drain_items(origin, carry):
        for c in range(nc + ns):
            @pl.when((origin <= z) & can_up)
            def _():
                copy(c, origin, UP).wait_send()

            @pl.when((origin >= z) & can_down)
            def _():
                copy(c, origin, DOWN).wait_send()

        for s in range(ns):
            for role in (OWN, OTHER):
                parity = parity_of(role)
                hand(s, origin, role, parity).wait_send()
                for step in range(1, pairs):
                    far(s, origin, role, parity, step).wait_send()
            back(s, origin, x).wait_send()
        return carry

    lax.fori_loop(0, nz, drain_items, 0)
    across().wait_send()
    for parity in (x, 1 - x):
        for step in range(1, pairs):
            to_far(parity, step).wait_send()
        for step in range(pairs):
            to_mate(parity, lax.rem(mp + 2 * step, n_mp)).wait_send()
    for c in range(nc):
        swap(c).wait_send()
    for j in range(nq):
        share(j, x).wait_send()
    for out in [out_k, out_v] + outs:
        out.wait()


def local(n_dp, n_mp, hidden, lengths, norm_gain, w_query, w_key, w_value, w_out, post_gain):
    _, local_len, width = hidden.shape
    maxlen = local_len * n_mp
    rows, qw = w_query.shape
    kw = w_key.shape[1]
    orows, fcols = w_out.shape
    nz, pairs = n_dp // 2, n_mp // 2
    far = max(1, pairs - 1)
    nq = qw // kw
    nc = 2 + nq
    pieces = cut(fcols)
    ns = len(pieces)
    cosine, sine = tables(maxlen)
    anywhere = pl.BlockSpec(memory_space=pl.ANY)
    bf16, f32 = jnp.bfloat16, jnp.float32
    dma = pltpu.SemaphoreType.DMA
    tiles = (width // LANES, LANES)

    def per_piece(*lead):
        return [pltpu.VMEM((*lead, local_len, size), bf16) for _, size in pieces]

    mixed, keys, values = pl.pallas_call(
        functools.partial(kernel, n_dp, n_mp, pieces),
        out_shape=(
            jax.ShapeDtypeStruct((local_len, width), bf16),
            jax.ShapeDtypeStruct((maxlen, kw), bf16),
            jax.ShapeDtypeStruct((maxlen, kw), bf16),
        ),
        in_specs=[pl.BlockSpec(memory_space=pltpu.SMEM)] + [anywhere] * 9,
        out_specs=(anywhere,) * 3,
        scratch_shapes=[
            pltpu.VMEM((local_len, width), bf16),
            pltpu.VMEM(tiles, f32),
            pltpu.VMEM(tiles, f32),
            pltpu.VMEM((1, width), f32),
            pltpu.VMEM((1, width), f32),
            pltpu.VMEM((maxlen, HD), f32),
            pltpu.VMEM((maxlen, HD), f32),
            pltpu.VMEM((nz, nc, rows, kw), bf16),
            pltpu.VMEM((nz, fcols, orows), bf16),
            pltpu.VMEM((nz, 2 * maxlen + local_len, rows), bf16),
            pltpu.VMEM((nc, 2 * maxlen, kw), f32),
            pltpu.VMEM((nc, maxlen, kw), bf16),
            pltpu.VMEM((nc, maxlen, kw), bf16),
            pltpu.VMEM((maxlen, kw), bf16),
            pltpu.VMEM((maxlen, kw), bf16),
            pltpu.VMEM((kw // HD, maxlen, 2 * HD), bf16),
            pltpu.VMEM((2, maxlen, qw), bf16),
            pltpu.VMEM((local_len, 1), f32),
            pltpu.VMEM((local_len, width), bf16),
            *per_piece(nz, 2, 2, pairs),
            *per_piece(nz, 2, pairs),
            *per_piece(nz, 2, far),
            *per_piece(nz),
            *per_piece(2, nz),
            dma((nc + 6,)),
            dma((nc + ns, 2, nz)),
            dma((nc + ns, nz)),
            dma((1,)),
            dma((2, pairs)),
            dma((2, far)),
            dma((2, n_mp)),
            dma((nc,)),
            dma((nc,)),
            dma((nq,)),
            dma((nq,)),
            dma((ns, nz, 2)),
            dma((ns, nz, 2)),
            dma((ns, nz, 2, far)),
            dma((ns, nz, 2, far)),
            dma((ns, nz)),
            dma((ns, nz)),
            dma((4,)),
        ],
        compiler_params=pltpu.CompilerParams(
            collective_id=0, has_side_effects=True, vmem_limit_bytes=60 * 1024 * 1024
        ),
    )(
        lengths,
        hidden[0],
        norm_gain.reshape(tiles),
        w_query,
        w_key,
        w_value,
        w_out.T,
        post_gain.reshape(tiles),
        jnp.asarray(cosine),
        jnp.asarray(sine),
    )
    return mixed[None], keys[None], values[None]


def solution(mesh):
    return jax.shard_map(
        functools.partial(local, mesh.shape["dp"], mesh.shape["mp"]),
        mesh=mesh,
        in_specs=(
            P("dp", "mp", None),
            P("dp"),
            P(),
            P("dp", "mp"),
            P("dp", "mp"),
            P("dp", "mp"),
            P("mp", "dp"),
            P(),
        ),
        out_specs=(P("dp", "mp", None), P("dp", None, "mp"), P("dp", None, "mp")),
        check_vma=False,
    )
```

```python
import functools

import jax
import jax.numpy as jnp
import numpy as np
from jax import lax
from jax.experimental import pallas as pl
from jax.experimental.pallas import tpu as pltpu
from jax.sharding import PartitionSpec as P

HD = 128
LANES = 128
MESH = pl.DeviceIdType.MESH
UP, DOWN = 0, 1
OWN, OTHER = 0, 1


def tables(maxlen):
    half = HD // 2
    freqs = 10000.0 ** (-np.arange(half, dtype=np.float64) / half)
    angles = np.arange(maxlen, dtype=np.float64)[:, None] * freqs[None, :]
    cosine, sine = np.cos(angles), np.sin(angles)
    return (
        np.concatenate([cosine, cosine], axis=1).astype(np.float32),
        np.concatenate([-sine, sine], axis=1).astype(np.float32),
    )


def cut(rows):
    pieces, start = [], 0
    while start < rows:
        size = min(256, rows - start)
        pieces.append((start, size))
        start += size
    return pieces


def kernel(
    n_dp, n_mp, pieces,
    len_ref, hid_in, ngain_in, wq, wk, wv, wo, pgain_in, cos_in, sin_in,
    mbuf, kbuf, vbuf,
    *scratch,
):
    ns = len(pieces)
    (
        hid, ngain_t, pgain_t, ngain, pgain, cos_ref, sin_ref,
        wbuf, obuf, nbuf, acc, pout, pin, vext, att, sq,
        hrows, hacc, hpout, hpin, hsum, epin,
    ) = scratch[:22]
    rest = scratch[22:]
    psend, inbox, precv, xout, yall = (rest[i * ns : (i + 1) * ns] for i in range(5))
    (
        load_sem, zsend, zrecv, xsend, xmate, xfar, xrecv, qsend, qrecv, asend, arecv,
        hsend, hrecv, fsend, frecv, csend, crecv,
        lsend, lmate, lfar, lrecv, bsend, brecv, esend, erecv,
    ) = rest[5 * ns :]

    nz = n_dp // 2
    pairs = n_mp // 2
    me, mp = lax.axis_index("dp"), lax.axis_index("mp")
    z, x = me // 2, me % 2
    side, slot = mp % 2, mp // 2
    partner = me + 1 - 2 * x
    mate = mp + 1 - 2 * side
    local_len, width = hid.shape
    maxlen = local_len * n_mp
    fcols = width // n_dp
    rows_each = wq.shape[0]
    qw, kw = wq.shape[1], wk.shape[1]
    nq = qw // kw
    nc = 2 + nq
    at_k, at_v = 1, 2
    at_q = [0] + list(range(3, nc))
    lent = (at_k, at_v)
    half = nz // 2
    q_heads, kv_heads = qw // HD, kw // HD
    can_up, can_down = z < nz - 1, z > 0
    middle = can_up & can_down
    ends = jnp.logical_not(middle)
    helps = (z == 1) | (z == nz - 2)
    far_half = jnp.where((z == 0) | (z == 1), 1, 0)
    inward = jnp.where(z == 0, me + 2, me - 2)
    outward = jnp.where(z == 1, me - 2, me + 2)
    f32, bf16 = jnp.float32, jnp.bfloat16

    def remote(src, dst, send, recv, dp_index, mp_index):
        return pltpu.make_async_remote_copy(
            src_ref=src, dst_ref=dst, send_sem=send, recv_sem=recv,
            device_id=(dp_index, mp_index), device_id_type=MESH,
        )

    def item(c, origin):
        if c < nc:
            first = pl.multiple_of(origin % half * rows_each, rows_each)
            return wbuf.at[c, origin // half, pl.ds(first, rows_each)]
        start, size = pieces[c - nc]
        return obuf.at[origin, pl.ds(start, size)]

    sources = [None] * nc
    sources[at_k], sources[at_v] = wk, wv
    for j, c in enumerate(at_q):
        sources[c] = wq.at[:, pl.ds(j * kw, kw)]
    load_w = [
        pltpu.make_async_copy(source, item(c, z), load_sem.at[c])
        for c, source in enumerate(sources)
    ]
    load_o = pltpu.make_async_copy(wo, obuf.at[z], load_sem.at[nc])
    load_x = [
        pltpu.make_async_copy(hid_in, hid, load_sem.at[nc + 1]),
        pltpu.make_async_copy(ngain_in, ngain_t, load_sem.at[nc + 2]),
    ]
    load_r = [
        pltpu.make_async_copy(pgain_in, pgain_t, load_sem.at[nc + 3]),
        pltpu.make_async_copy(cos_in, cos_ref, load_sem.at[nc + 4]),
        pltpu.make_async_copy(sin_in, sin_ref, load_sem.at[nc + 5]),
    ]
    for load in load_w[:1] + load_x + load_w[1:] + [load_o] + load_r:
        load.start()

    barrier = pltpu.get_barrier_semaphore()

    def greet(dp_index, mp_index):
        pl.semaphore_signal(barrier, inc=1, device_id=(dp_index, mp_index), device_id_type=MESH)

    greet(partner, mp)
    for step in range(1, n_mp):
        greet(me, lax.rem(mp + step, n_mp))

    @pl.when(can_up)
    def _():
        greet(me + 2, mp)

    @pl.when(can_down)
    def _():
        greet(me - 2, mp)

    pl.semaphore_wait(
        barrier, n_mp + jnp.where(can_up, 1, 0) + jnp.where(can_down, 1, 0)
    )

    def copy(c, origin, way):
        ref = item(c, origin)
        return remote(
            ref, ref, zsend.at[1 if c in lent else 0, way, origin], zrecv.at[c, origin],
            (me + 2, me - 2)[way], mp,
        )

    def sends(c, origin, way):
        if way == UP:
            skip, able = (z + 1 == nz - 1) & (origin < half), can_up
        else:
            skip, able = (z - 1 == 0) & (origin >= half), can_down
        return able & jnp.logical_not(skip) if c in lent else able

    def gets(c, origin):
        if c not in lent:
            return (origin >= 0) & (origin < nz)
        low, high = jnp.where(z == nz - 1, half, 0), jnp.where(z == 0, half, nz)
        return (origin >= low) & (origin < high)

    def send(c, origin, way):
        @pl.when(sends(c, origin, way))
        def _():
            copy(c, origin, way).start()

    def send_own(c):
        send(c, z, UP)
        send(c, z, DOWN)

    def send_own_out(c, down, up):
        @pl.when(down & middle)
        def _():
            copy(c, z, DOWN).start()

        @pl.when(up & middle)
        def _():
            copy(c, z, UP).start()

    def relay(c, k):
        for origin, way in ((z - k, UP), (z + k, DOWN)):
            @pl.when(gets(c, origin))
            def _():
                copy(c, origin, way).wait_recv()
                send(c, origin, way)

    def relays(c, first, last):
        def body(k, carry):
            relay(c, k)
            return carry

        lax.fori_loop(first, last, body, 0)

    def rows_of(parity, block):
        return pl.ds(pl.multiple_of(parity * maxlen + block * local_len, local_len), local_len)

    def region(parity, block):
        return nbuf.at[:, rows_of(parity, block), :]

    def across():
        return remote(
            nbuf.at[:, pl.ds(2 * maxlen, local_len), :], region(x, mp),
            xsend.at[0], xrecv.at[x, mp], partner, mp,
        )

    def to_mate(parity, block):
        return remote(
            region(parity, block), region(parity, block),
            xmate.at[parity, block // 2], xrecv.at[parity, block], me, mate,
        )

    def to_far(parity, step):
        return remote(
            region(parity, mp), region(parity, mp),
            xfar.at[parity, step - 1], xrecv.at[parity, mp], me, lax.rem(mp + 2 * step, n_mp),
        )

    def arrived(parity, block):
        return remote(
            region(parity, block), region(parity, block),
            xsend.at[0], xrecv.at[parity, block], me, mate,
        )

    def spread(parity):
        for step in range(1, pairs):
            to_far(parity, step).start()
        to_mate(parity, mp).start()

    def pass_on(parity):
        for step in range(1, pairs):
            block = lax.rem(mp + 2 * step, n_mp)
            arrived(parity, block).wait_recv()
            to_mate(parity, block).start()

    def lend(parity):
        return remote(
            nbuf.at[far_half, rows_of(parity, mp), :],
            hrows.at[rows_of(parity, mp), :],
            lsend.at[parity], lrecv.at[parity, mp], inward, mp,
        )

    def lent_to(parity, block, dst, send_sem):
        ref = hrows.at[rows_of(parity, block), :]
        return remote(ref, ref, send_sem, lrecv.at[parity, block], me, dst)

    def lent_mate(parity, block):
        return lent_to(parity, block, mate, lmate.at[parity, block // 2])

    def lent_far(parity, step):
        return lent_to(parity, mp, lax.rem(mp + 2 * step, n_mp), lfar.at[parity, step - 1])

    def lent_wait(parity, block):
        lent_to(parity, block, mate, lsend.at[parity]).wait_recv()

    def lent_spread(parity):
        lent_wait(parity, mp)
        for step in range(1, pairs):
            lent_far(parity, step).start()
        lent_mate(parity, mp).start()

    def lent_pass(parity):
        for step in range(1, pairs):
            block = lax.rem(mp + 2 * step, n_mp)
            lent_wait(parity, block)
            lent_mate(parity, block).start()

    load_w[0].wait()
    send_own(0)
    for load in load_x:
        load.wait()
    for t in range(width // LANES):
        ngain[:, t * LANES : (t + 1) * LANES] = ngain_t[t : t + 1, :]
    total = jnp.zeros((local_len, LANES), f32)
    for t in range(width // LANES):
        rows = hid[:, t * LANES : (t + 1) * LANES].astype(f32)
        total = total + rows * rows
    scale = lax.rsqrt(jnp.sum(total, axis=-1, keepdims=True) / width + 1e-06)
    for block in range(n_dp):
        span = slice(block * fcols, (block + 1) * fcols)
        rows = hid[:, span].astype(f32)
        first = jnp.where(x == block % 2, x * maxlen + mp * local_len, 2 * maxlen)
        k = block // 2
        cols = slice(k % half * fcols, (k % half + 1) * fcols)
        nbuf[k // half, pl.ds(pl.multiple_of(first, local_len), local_len), cols] = (
            rows * scale * ngain[:, span]
        ).astype(bf16)
    across().start()
    spread(x)

    @pl.when(ends)
    def _():
        lend(x).start()

    load_w[1].wait()
    send_own(1)
    acc[...] = jnp.zeros_like(acc)

    @pl.when(middle)
    def _():
        epin[...] = jnp.zeros_like(epin)

    def rollout_rows(parity):
        return pl.ds(pl.multiple_of(parity * maxlen, maxlen), maxlen)

    def swap(c):
        return remote(pout.at[c], pin.at[c], qsend.at[c], qrecv.at[c], partner, mp)

    def compute(c):
        first, last = 0, 2
        if c in lent:
            first, last = jnp.where(z == nz - 1, 1, 0), jnp.where(z == 0, 1, 2)

        def contract(parity):
            rows = rollout_rows(parity)

            def body(k, carry):
                acc[c, rows, :] += jnp.dot(
                    nbuf[k, rows, :], wbuf[c, k], preferred_element_type=f32
                )
                return carry

            lax.fori_loop(first, last, body, 0)

        contract(1 - x)
        pout[c] = acc[c, rollout_rows(1 - x), :].astype(bf16)
        swap(c).start()
        contract(x)

    def lent_swap(i):
        return remote(hpout.at[i], hpin.at[i], bsend.at[i], brecv.at[i], partner, mp)

    def lent_return(i):
        return remote(hsum.at[i], epin.at[i], esend.at[i], erecv.at[i], outward, mp)

    def lent_compute(i):
        def contract(parity):
            rows = rollout_rows(parity)

            hacc[i, rows, :] = jnp.dot(
                hrows[rows, :], wbuf[lent[i], far_half], preferred_element_type=f32
            )

        contract(1 - x)
        hpout[i] = hacc[i, rollout_rows(1 - x), :].astype(bf16)
        lent_swap(i).start()
        contract(x)

    def lent_finish(i):
        lent_swap(i).wait_recv()
        hsum[i] = (hacc[i, rollout_rows(x), :] + hpin[i].astype(f32)).astype(bf16)
        lent_return(i).start()

    def lent_add(i, cols):
        return epin[i, :, cols].astype(f32)

    def lent_ready(i):
        @pl.when(ends)
        def _():
            lent_return(i).wait_recv()

    length = len_ref[0]
    live = lax.broadcasted_iota(jnp.int32, (maxlen, HD), 0) < length

    def rotated(block, span):
        return block * cos_ref[span, :] + pltpu.roll(block, HD // 2, 1) * sin_ref[span, :]

    everything = slice(0, maxlen)

    def keys_done():
        swap(at_k).wait_recv()
        lent_ready(0)
        for h in range(kv_heads):
            cols = slice(h * HD, (h + 1) * HD)
            raw = acc[at_k, rollout_rows(x), cols] + pin[at_k, :, cols].astype(f32)
            raw = raw + lent_add(0, cols)
            kbuf[:, cols] = jnp.where(live, rotated(raw, everything), 0.0).astype(bf16)

    def values_done():
        swap(at_v).wait_recv()
        lent_ready(1)
        for h in range(kv_heads):
            cols = slice(h * HD, (h + 1) * HD)
            raw = acc[at_v, rollout_rows(x), cols] + pin[at_v, :, cols].astype(f32)
            raw = raw + lent_add(1, cols)
            value = jnp.where(live, raw, 0.0).astype(bf16)
            vbuf[:, cols] = value
            vext[h, :, :HD] = value
            vext[h, :, HD:] = jnp.where(live, 1.0, 0.0).astype(bf16)

    def share(j, parity):
        ref = att.at[parity, :, pl.ds(j * kw, kw)]
        return remote(ref, ref, asend.at[j], arecv.at[j], partner, mp)

    def attend(j):
        swap(at_q[j]).wait_recv()
        for i in range(kv_heads):
            h = j * kv_heads + i
            kv = h * kv_heads // q_heads
            cols, kcols = slice(i * HD, (i + 1) * HD), slice(kv * HD, (kv + 1) * HD)
            for r in range(n_mp):
                span, seen = slice(r * local_len, (r + 1) * local_len), (r + 1) * local_len
                raw = acc[at_q[j], rows_of(x, r), cols] + pin[at_q[j], span, cols].astype(f32)
                query = (rotated(raw, span) * 144.0 ** (-0.5)).astype(bf16)
                score = lax.dot_general(
                    query, kbuf[:seen, kcols], (((1,), (1,)), ((), ())),
                    preferred_element_type=f32,
                )
                row = lax.broadcasted_iota(jnp.int32, score.shape, 0) + r * local_len
                col = lax.broadcasted_iota(jnp.int32, score.shape, 1)
                expo = jnp.exp2(jnp.tanh(score * (1.0 / 50.0)) * (50.0 * np.log2(np.e)))
                expo = jnp.where(col <= row, expo, 0.0).astype(bf16)
                both = jnp.dot(expo, vext[kv, :seen, :], preferred_element_type=f32)
                att[x, span, h * HD : (h + 1) * HD] = (both[:, :HD] / both[:, HD:]).astype(bf16)
        share(j, x).start()

    relays(0, 1, 2)
    arrived(1 - x, mp).wait_recv()
    spread(1 - x)

    @pl.when(ends)
    def _():
        lend(1 - x).start()

    for load in load_w[2:] + [load_o]:
        load.wait()
    send_own(2)

    @pl.when(ends)
    def _():
        for c in range(3, nc + ns):
            send_own(c)

    pass_on(x)

    @pl.when(helps)
    def _():
        lent_spread(x)

    relays(0, 2, nz)
    relays(1, 1, 2)
    @pl.when(middle)
    def _():
        for c in range(3, nc):
            send_own(c)

    early = {0, ns - 1}
    for s in sorted(early):
        send_own_out(nc + s, z == 1, z == nz - 2)

    @pl.when(helps)
    def _():
        lent_spread(1 - x)

    pass_on(1 - x)
    for parity in (x, 1 - x):
        for step in range(pairs):
            arrived(parity, lax.rem(mate + 2 * step, n_mp)).wait_recv()
    compute(0)

    @pl.when(helps)
    def _():
        lent_pass(x)

    relays(1, 2, nz)
    relays(2, 1, 2)
    compute(1)

    @pl.when(helps)
    def _():
        lent_pass(1 - x)
        for parity in (x, 1 - x):
            for step in range(pairs):
                lent_wait(parity, lax.rem(mate + 2 * step, n_mp))
        lent_compute(0)

    for c in range(3, nc):
        relays(c, 1, 2)
    for load in load_r:
        load.wait()
    for t in range(width // LANES):
        pgain[:, t * LANES : (t + 1) * LANES] = pgain_t[t : t + 1, :]
    relays(2, 2, nz)

    @pl.when(helps)
    def _():
        lent_compute(1)

    compute(2)

    @pl.when(helps)
    def _():
        lent_finish(0)

    for c in range(3, nc):
        relays(c, 2, nz)
        compute(c)

    @pl.when(helps)
    def _():
        lent_finish(1)

    for s in range(ns):
        sent_out = s in early
        send_own_out(nc + s, z != 1 if sent_out else True, z != nz - 2 if sent_out else True)

    keys_done()
    values_done()
    for j in range(nq - 1):
        attend(j)

    def hand(s, zk, role, parity):
        return remote(
            psend[s].at[zk, parity, 1 - side], inbox[s].at[zk, parity],
            hsend.at[s], hrecv.at[s, zk, role], me, mate,
        )

    def far(s, zk, role, parity, step):
        target = lax.rem(mp + 2 * step, n_mp)
        return remote(
            psend[s].at[zk, parity, side, target // 2], precv[s].at[zk, parity, step - 1],
            fsend.at[s], frecv.at[s, zk, role, step - 1], me, target,
        )

    def back(s, zk, parity):
        return remote(
            xout[s].at[zk], yall[s].at[parity, zk], csend.at[s], crecv.at[s], partner, mp
        )

    def parity_of(role):
        return x if role == OWN else 1 - x

    def produce(s, zk, role):
        start, size = pieces[s]
        parity = parity_of(role)
        part = lax.dot_general(
            att[parity], obuf[zk, start : start + size, :], (((1,), (1,)), ((), ())),
            preferred_element_type=f32,
        ).astype(bf16)
        for p in range(n_mp):
            psend[s][zk, parity, p % 2, p // 2] = part[p * local_len : (p + 1) * local_len]
        hand(s, zk, role, parity).start()

    def combine(s, zk, role):
        parity = parity_of(role)
        hand(s, zk, role, parity).wait_recv()
        for step in range(1, pairs):
            q = lax.rem(mp + 2 * step, n_mp) // 2
            both = psend[s][zk, parity, side, q].astype(f32) + inbox[s][zk, parity, q].astype(f32)
            psend[s][zk, parity, side, q] = both.astype(bf16)
            far(s, zk, role, parity, step).start()

    def measure(value):
        value = value.astype(f32)
        sq[...] += jnp.sum(value * value, axis=-1, keepdims=True)

    def settle(s, zk, role):
        parity = parity_of(role)
        value = psend[s][zk, parity, side, slot].astype(f32)
        value = value + inbox[s][zk, parity, slot].astype(f32)
        for step in range(1, pairs):
            far(s, zk, role, parity, step).wait_recv()
            value = value + precv[s][zk, parity, step - 1].astype(f32)
        value = value.astype(bf16)
        if role == OWN:
            yall[s][x, zk] = value
            measure(value)
        else:
            xout[s][zk] = value
            back(s, zk, x).start()

    def around(k, act):
        def body(way, carry):
            zk = z + k * (2 * way - 1)

            @pl.when((zk >= 0) & (zk < nz) & ((way == 0) | (k > 0)))
            def _():
                act(zk)

            return carry

        lax.fori_loop(0, 2, body, 0)

    def near(act):
        def body(k, carry):
            around(k, act)
            return carry

        lax.fori_loop(0, min(2, nz), body, 0)

    attend(nq - 1)
    sq[...] = jnp.zeros_like(sq)
    for s in range(ns):
        produce(s, z, OWN)
    for s in range(ns):
        relays(nc + s, 1, 2)
        combine(s, z, OWN)
    for s in range(ns):
        around(1, functools.partial(produce, s, role=OWN))
    for s in range(ns):
        around(1, functools.partial(combine, s, role=OWN))
    for j in range(nq):
        share(j, 1 - x).wait_recv()
    for s in range(ns):
        near(functools.partial(produce, s, role=OTHER))
    for s in range(ns):
        near(functools.partial(combine, s, role=OTHER))

    def settle_near():
        for role in (OTHER, OWN):
            for s in range(ns):
                near(functools.partial(settle, s, role=role))

    def settle_at(s, k):
        def both(zk):
            for role in (OTHER, OWN):
                settle(s, zk, role)

        around(k, both)

    def late(k, carry):
        for s in range(ns):
            relay(nc + s, k)

            def make(zk, s=s):
                for role in (OTHER, OWN):
                    produce(s, zk, role)

            def join(zk, s=s):
                for role in (OTHER, OWN):
                    combine(s, zk, role)

            around(k, make)
            around(k, join)
            if s > 0:
                settle_at(s - 1, k)
            else:
                @pl.when(k == 2)
                def _():
                    settle_near()

                @pl.when(k > 2)
                def _():
                    settle_at(ns - 1, k - 1)

        return carry

    if nz > 2:
        lax.fori_loop(2, nz, late, 0)
        settle_at(ns - 1, nz - 1)
    else:
        settle_near()

    for s in range(ns):
        remote(xout[s], yall[s].at[1 - x], csend.at[s], crecv.at[s], partner, mp).wait_recv()

    def collect(zk, carry):
        for s in range(ns):
            measure(yall[s][1 - x, zk])
        return carry

    lax.fori_loop(0, nz, collect, 0)

    scale = lax.rsqrt(sq[...] / width + 1e-06)
    for block in range(n_dp):
        for s, (start, size) in enumerate(pieces):
            span = slice(block * fcols + start, block * fcols + start + size)
            own = lax.broadcasted_iota(jnp.int32, (local_len, size), 0) + mp * local_len < length
            post = yall[s][block % 2, block // 2].astype(f32) * scale * pgain[:, span]
            mbuf[:, span] = jnp.where(own, hid[:, span].astype(f32) + post, 0.0).astype(bf16)

    def sent(ref, sem):
        remote(ref, ref, sem, sem, partner, mp).wait_send()

    def drain_items(origin, carry):
        for way, mine in ((UP, origin <= z), (DOWN, origin >= z)):
            @pl.when(mine & sends(nc, origin, way))
            def _():
                sent(obuf.at[pl.ds(0, 2)], zsend.at[0, way, origin])

            @pl.when(mine & sends(at_k, origin, way))
            def _():
                sent(wbuf.at[pl.ds(at_k, 2), 0, pl.ds(0, rows_each)], zsend.at[1, way, origin])

        return carry

    lax.fori_loop(0, nz, drain_items, 0)
    for s in range(ns):
        sent(psend[s].at[:, :, 0], hsend.at[s])
        if pairs > 1:
            sent(precv[s], fsend.at[s])
        sent(xout[s], csend.at[s])
    across().wait_send()
    for parity in (x, 1 - x):
        for step in range(1, pairs):
            to_far(parity, step).wait_send()
        for step in range(pairs):
            to_mate(parity, lax.rem(mp + 2 * step, n_mp)).wait_send()
    for c in range(nc):
        swap(c).wait_send()

    @pl.when(ends)
    def _():
        for parity in range(2):
            lend(parity).wait_send()

    @pl.when(helps)
    def _():
        for parity in (x, 1 - x):
            for step in range(1, pairs):
                lent_far(parity, step).wait_send()
            for step in range(pairs):
                lent_mate(parity, lax.rem(mp + 2 * step, n_mp)).wait_send()
        for i in range(len(lent)):
            lent_swap(i).wait_send()
            lent_return(i).wait_send()

    for j in range(nq):
        share(j, x).wait_send()


def local(n_dp, n_mp, hidden, lengths, norm_gain, w_query, w_key, w_value, w_out, post_gain):
    _, local_len, width = hidden.shape
    maxlen = local_len * n_mp
    rows, qw = w_query.shape
    kw = w_key.shape[1]
    orows, fcols = w_out.shape
    nz, pairs = n_dp // 2, n_mp // 2
    far = max(1, pairs - 1)
    nq = qw // kw
    nc = 2 + nq
    pieces = cut(fcols)
    ns = len(pieces)
    cosine, sine = tables(maxlen)
    anywhere = pl.BlockSpec(memory_space=pl.ANY)
    bf16, f32 = jnp.bfloat16, jnp.float32
    dma = pltpu.SemaphoreType.DMA
    tiles = (width // LANES, LANES)

    def per_piece(*lead):
        return [pltpu.VMEM((*lead, local_len, size), bf16) for _, size in pieces]

    mixed, keys, values = pl.pallas_call(
        functools.partial(kernel, n_dp, n_mp, pieces),
        out_shape=(
            pltpu.VMEM((local_len, width), bf16),
            pltpu.VMEM((maxlen, kw), bf16),
            pltpu.VMEM((maxlen, kw), bf16),
        ),
        in_specs=[pl.BlockSpec(memory_space=pltpu.SMEM)] + [anywhere] * 9,
        out_specs=(pl.BlockSpec(memory_space=pltpu.VMEM),) * 3,
        scratch_shapes=[
            pltpu.VMEM((local_len, width), bf16),
            pltpu.VMEM(tiles, f32),
            pltpu.VMEM(tiles, f32),
            pltpu.VMEM((1, width), f32),
            pltpu.VMEM((1, width), f32),
            pltpu.VMEM((maxlen, HD), f32),
            pltpu.VMEM((maxlen, HD), f32),
            pltpu.VMEM((nc, 2, nz // 2 * rows, kw), bf16),
            pltpu.VMEM((nz, fcols, orows), bf16),
            pltpu.VMEM((2, 2 * maxlen + local_len, nz // 2 * rows), bf16),
            pltpu.VMEM((nc, 2 * maxlen, kw), f32),
            pltpu.VMEM((nc, maxlen, kw), bf16),
            pltpu.VMEM((nc, maxlen, kw), bf16),
            pltpu.VMEM((kw // HD, maxlen, 2 * HD), bf16),
            pltpu.VMEM((2, maxlen, qw), bf16),
            pltpu.VMEM((local_len, 1), f32),
            pltpu.VMEM((2 * maxlen, nz // 2 * rows), bf16),
            pltpu.VMEM((2, 2 * maxlen, kw), f32),
            pltpu.VMEM((2, maxlen, kw), bf16),
            pltpu.VMEM((2, maxlen, kw), bf16),
            pltpu.VMEM((2, maxlen, kw), bf16),
            pltpu.VMEM((2, maxlen, kw), bf16),
            *per_piece(nz, 2, 2, pairs),
            *per_piece(nz, 2, pairs),
            *per_piece(nz, 2, far),
            *per_piece(nz),
            *per_piece(2, nz),
            dma((nc + 6,)),
            dma((2, 2, nz)),
            dma((nc + ns, nz)),
            dma((1,)),
            dma((2, pairs)),
            dma((2, far)),
            dma((2, n_mp)),
            dma((nc,)),
            dma((nc,)),
            dma((nq,)),
            dma((nq,)),
            dma((ns,)),
            dma((ns, nz, 2)),
            dma((ns,)),
            dma((ns, nz, 2, far)),
            dma((ns,)),
            dma((ns,)),
            dma((2,)),
            dma((2, pairs)),
            dma((2, far)),
            dma((2, n_mp)),
            dma((2,)),
            dma((2,)),
            dma((2,)),
            dma((2,)),
        ],
        compiler_params=pltpu.CompilerParams(
            collective_id=0, has_side_effects=True, vmem_limit_bytes=60 * 1024 * 1024
        ),
    )(
        lengths,
        hidden[0],
        norm_gain.reshape(tiles),
        w_query,
        w_key,
        w_value,
        w_out.T,
        post_gain.reshape(tiles),
        jnp.asarray(cosine),
        jnp.asarray(sine),
    )
    return mixed[None], keys[None], values[None]


def solution(mesh):
    return jax.shard_map(
        functools.partial(local, mesh.shape["dp"], mesh.shape["mp"]),
        mesh=mesh,
        in_specs=(
            P("dp", "mp", None),
            P("dp"),
            P(),
            P("dp", "mp"),
            P("dp", "mp"),
            P("dp", "mp"),
            P("mp", "dp"),
            P(),
        ),
        out_specs=(P("dp", "mp", None), P("dp", None, "mp"), P("dp", None, "mp")),
        check_vma=False,
    )
```

```python
import functools

import jax
import jax.numpy as jnp
import numpy as np
from jax import lax
from jax.experimental import pallas as pl
from jax.experimental.pallas import tpu as pltpu
from jax.sharding import PartitionSpec as P

HD = 128
LANES = 128
MESH = pl.DeviceIdType.MESH
UP, DOWN = 0, 1
OWN, OTHER = 0, 1


def tables(maxlen):
    half = HD // 2
    freqs = 10000.0 ** (-np.arange(half, dtype=np.float64) / half)
    angles = np.arange(maxlen, dtype=np.float64)[:, None] * freqs[None, :]
    cosine, sine = np.cos(angles), np.sin(angles)
    return (
        np.concatenate([cosine, cosine], axis=1).astype(np.float32),
        np.concatenate([-sine, sine], axis=1).astype(np.float32),
    )


def cut(rows):
    pieces, start = [], 0
    while start < rows:
        size = min(256, rows - start)
        pieces.append((start, size))
        start += size
    return pieces


def kernel(
    n_dp, n_mp, pieces,
    len_ref, hid_in, ngain_in, wq, wk, wv, wo, pgain_in, cos_in, sin_in,
    mbuf, kbuf, vbuf,
    *scratch,
):
    ns = len(pieces)
    (
        hid, ngain_t, pgain_t, ngain, pgain, cos_ref, sin_ref,
        wbuf, obuf, nbuf, acc, pout, pin, vext, att, sq,
        hrows, hacc, hpout, hpin, hsum, epin,
    ) = scratch[:22]
    rest = scratch[22:]
    psend, inbox, precv, xout, yall = (rest[i * ns : (i + 1) * ns] for i in range(5))
    (
        load_sem, zsend, zrecv, xsend, xmate, xfar, xrecv, qsend, qrecv, asend, arecv,
        hsend, hrecv, fsend, frecv, csend, crecv,
        lsend, lmate, lfar, lrecv, bsend, brecv, esend, erecv,
    ) = rest[5 * ns :]

    nz = n_dp // 2
    pairs = n_mp // 2
    me, mp = lax.axis_index("dp"), lax.axis_index("mp")
    z, x = me // 2, me % 2
    side, slot = mp % 2, mp // 2
    partner = me + 1 - 2 * x
    mate = mp + 1 - 2 * side
    local_len, width = hid.shape
    maxlen = local_len * n_mp
    fcols = width // n_dp
    rows_each = wq.shape[0]
    qw, kw = wq.shape[1], wk.shape[1]
    nq = qw // kw
    nc = 2 + nq
    at_k, at_v = 1, 2
    at_q = [0] + list(range(3, nc))
    lent = (at_k, at_v)
    half = nz // 2
    q_heads, kv_heads = qw // HD, kw // HD
    can_up, can_down = z < nz - 1, z > 0
    middle = can_up & can_down
    ends = jnp.logical_not(middle)
    helps = (z == 1) | (z == nz - 2)
    far_half = jnp.where((z == 0) | (z == 1), 1, 0)
    inward = jnp.where(z == 0, me + 2, me - 2)
    outward = jnp.where(z == 1, me - 2, me + 2)
    f32, bf16 = jnp.float32, jnp.bfloat16

    def remote(src, dst, send, recv, dp_index, mp_index):
        return pltpu.make_async_remote_copy(
            src_ref=src, dst_ref=dst, send_sem=send, recv_sem=recv,
            device_id=(dp_index, mp_index), device_id_type=MESH,
        )

    def item(c, origin):
        if c < nc:
            first = pl.multiple_of(origin % half * rows_each, rows_each)
            return wbuf.at[c, origin // half, pl.ds(first, rows_each)]
        start, size = pieces[c - nc]
        return obuf.at[origin, pl.ds(start, size)]

    sources = [None] * nc
    sources[at_k], sources[at_v] = wk, wv
    for j, c in enumerate(at_q):
        sources[c] = wq.at[:, pl.ds(j * kw, kw)]
    load_w = [
        pltpu.make_async_copy(source, item(c, z), load_sem.at[c])
        for c, source in enumerate(sources)
    ]
    load_o = pltpu.make_async_copy(wo, obuf.at[z], load_sem.at[nc])
    load_x = [
        pltpu.make_async_copy(hid_in, hid, load_sem.at[nc + 1]),
        pltpu.make_async_copy(ngain_in, ngain_t, load_sem.at[nc + 2]),
    ]
    load_r = [
        pltpu.make_async_copy(pgain_in, pgain_t, load_sem.at[nc + 3]),
        pltpu.make_async_copy(cos_in, cos_ref, load_sem.at[nc + 4]),
        pltpu.make_async_copy(sin_in, sin_ref, load_sem.at[nc + 5]),
    ]
    for load in load_w[:1] + load_x + load_w[1:] + [load_o] + load_r:
        load.start()

    barrier = pltpu.get_barrier_semaphore()

    def greet(dp_index, mp_index):
        pl.semaphore_signal(barrier, inc=1, device_id=(dp_index, mp_index), device_id_type=MESH)

    greet(partner, mp)
    for step in range(1, n_mp):
        greet(me, lax.rem(mp + step, n_mp))

    @pl.when(can_up)
    def _():
        greet(me + 2, mp)

    @pl.when(can_down)
    def _():
        greet(me - 2, mp)

    pl.semaphore_wait(
        barrier, n_mp + jnp.where(can_up, 1, 0) + jnp.where(can_down, 1, 0)
    )

    def copy(c, origin, way):
        ref = item(c, origin)
        return remote(
            ref, ref, zsend.at[1 if c in lent else 0, way, origin], zrecv.at[c, origin],
            (me + 2, me - 2)[way], mp,
        )

    def sends(c, origin, way):
        if way == UP:
            skip, able = (z + 1 == nz - 1) & (origin < half), can_up
        else:
            skip, able = (z - 1 == 0) & (origin >= half), can_down
        return able & jnp.logical_not(skip) if c in lent else able

    def gets(c, origin):
        if c not in lent:
            return (origin >= 0) & (origin < nz)
        low, high = jnp.where(z == nz - 1, half, 0), jnp.where(z == 0, half, nz)
        return (origin >= low) & (origin < high)

    def send(c, origin, way):
        @pl.when(sends(c, origin, way))
        def _():
            copy(c, origin, way).start()

    def send_own(c):
        send(c, z, UP)
        send(c, z, DOWN)

    def send_own_out(c, down, up):
        @pl.when(down & middle)
        def _():
            copy(c, z, DOWN).start()

        @pl.when(up & middle)
        def _():
            copy(c, z, UP).start()

    def relay(c, k):
        for origin, way in ((z - k, UP), (z + k, DOWN)):
            @pl.when(gets(c, origin))
            def _():
                copy(c, origin, way).wait_recv()
                send(c, origin, way)

    def relays(c, first, last):
        def body(k, carry):
            relay(c, k)
            return carry

        lax.fori_loop(first, last, body, 0)

    def rows_of(parity, block):
        return pl.ds(pl.multiple_of(parity * maxlen + block * local_len, local_len), local_len)

    def region(parity, block):
        return nbuf.at[:, rows_of(parity, block), :]

    def across():
        return remote(
            nbuf.at[:, pl.ds(2 * maxlen, local_len), :], region(x, mp),
            xsend.at[0], xrecv.at[x, mp], partner, mp,
        )

    def to_mate(parity, block):
        return remote(
            region(parity, block), region(parity, block),
            xmate.at[parity, block // 2], xrecv.at[parity, block], me, mate,
        )

    def to_far(parity, step):
        return remote(
            region(parity, mp), region(parity, mp),
            xfar.at[parity, step - 1], xrecv.at[parity, mp], me, lax.rem(mp + 2 * step, n_mp),
        )

    def arrived(parity, block):
        return remote(
            region(parity, block), region(parity, block),
            xsend.at[0], xrecv.at[parity, block], me, mate,
        )

    def spread(parity):
        for step in range(1, pairs):
            to_far(parity, step).start()
        to_mate(parity, mp).start()

    def pass_on(parity):
        for step in range(1, pairs):
            block = lax.rem(mp + 2 * step, n_mp)
            arrived(parity, block).wait_recv()
            to_mate(parity, block).start()

    def lend(parity):
        return remote(
            nbuf.at[far_half, rows_of(parity, mp), :],
            hrows.at[rows_of(parity, mp), :],
            lsend.at[parity], lrecv.at[parity, mp], inward, mp,
        )

    def lent_to(parity, block, dst, send_sem):
        ref = hrows.at[rows_of(parity, block), :]
        return remote(ref, ref, send_sem, lrecv.at[parity, block], me, dst)

    def lent_mate(parity, block):
        return lent_to(parity, block, mate, lmate.at[parity, block // 2])

    def lent_far(parity, step):
        return lent_to(parity, mp, lax.rem(mp + 2 * step, n_mp), lfar.at[parity, step - 1])

    def lent_wait(parity, block):
        lent_to(parity, block, mate, lsend.at[parity]).wait_recv()

    def lent_spread(parity):
        lent_wait(parity, mp)
        for step in range(1, pairs):
            lent_far(parity, step).start()
        lent_mate(parity, mp).start()

    def lent_pass(parity):
        for step in range(1, pairs):
            block = lax.rem(mp + 2 * step, n_mp)
            lent_wait(parity, block)
            lent_mate(parity, block).start()

    load_w[0].wait()
    send_own(0)
    for load in load_x:
        load.wait()
    for t in range(width // LANES):
        ngain[:, t * LANES : (t + 1) * LANES] = ngain_t[t : t + 1, :]
    total = jnp.zeros((local_len, LANES), f32)
    for t in range(width // LANES):
        rows = hid[:, t * LANES : (t + 1) * LANES].astype(f32)
        total = total + rows * rows
    scale = lax.rsqrt(jnp.sum(total, axis=-1, keepdims=True) / width + 1e-06)
    for block in range(n_dp):
        span = slice(block * fcols, (block + 1) * fcols)
        rows = hid[:, span].astype(f32)
        first = jnp.where(x == block % 2, x * maxlen + mp * local_len, 2 * maxlen)
        k = block // 2
        cols = slice(k % half * fcols, (k % half + 1) * fcols)
        nbuf[k // half, pl.ds(pl.multiple_of(first, local_len), local_len), cols] = (
            rows * scale * ngain[:, span]
        ).astype(bf16)
    across().start()
    spread(x)

    @pl.when(ends)
    def _():
        lend(x).start()

    load_w[1].wait()
    send_own(1)
    acc[...] = jnp.zeros_like(acc)

    @pl.when(middle)
    def _():
        epin[...] = jnp.zeros_like(epin)

    def rollout_rows(parity):
        return pl.ds(pl.multiple_of(parity * maxlen, maxlen), maxlen)

    def swap(c):
        return remote(pout.at[c], pin.at[c], qsend.at[c], qrecv.at[c], partner, mp)

    def compute(c):
        first, last = 0, 2
        if c in lent:
            first, last = jnp.where(z == nz - 1, 1, 0), jnp.where(z == 0, 1, 2)

        def contract(parity):
            rows = rollout_rows(parity)

            def body(k, carry):
                acc[c, rows, :] += jnp.dot(
                    nbuf[k, rows, :], wbuf[c, k], preferred_element_type=f32
                )
                return carry

            lax.fori_loop(first, last, body, 0)

        contract(1 - x)
        pout[c] = acc[c, rollout_rows(1 - x), :].astype(bf16)
        swap(c).start()
        contract(x)

    def lent_swap(i):
        return remote(hpout.at[i], hpin.at[i], bsend.at[i], brecv.at[i], partner, mp)

    def lent_return(i):
        return remote(hsum.at[i], epin.at[i], esend.at[i], erecv.at[i], outward, mp)

    def lent_compute(i):
        def contract(parity):
            rows = rollout_rows(parity)

            hacc[i, rows, :] = jnp.dot(
                hrows[rows, :], wbuf[lent[i], far_half], preferred_element_type=f32
            )

        contract(1 - x)
        hpout[i] = hacc[i, rollout_rows(1 - x), :].astype(bf16)
        lent_swap(i).start()
        contract(x)

    def lent_finish(i):
        lent_swap(i).wait_recv()
        hsum[i] = (hacc[i, rollout_rows(x), :] + hpin[i].astype(f32)).astype(bf16)
        lent_return(i).start()

    def lent_add(i, cols):
        return epin[i, :, cols].astype(f32)

    def lent_ready(i):
        @pl.when(ends)
        def _():
            lent_return(i).wait_recv()

    length = len_ref[0]
    live = lax.broadcasted_iota(jnp.int32, (maxlen, HD), 0) < length

    def rotated(block, span):
        return block * cos_ref[span, :] + pltpu.roll(block, HD // 2, 1) * sin_ref[span, :]

    everything = slice(0, maxlen)

    def keys_done():
        swap(at_k).wait_recv()
        lent_ready(0)
        for h in range(kv_heads):
            cols = slice(h * HD, (h + 1) * HD)
            raw = acc[at_k, rollout_rows(x), cols] + pin[at_k, :, cols].astype(f32)
            raw = raw + lent_add(0, cols)
            kbuf[:, cols] = jnp.where(live, rotated(raw, everything), 0.0).astype(bf16)

    def values_done():
        swap(at_v).wait_recv()
        lent_ready(1)
        for h in range(kv_heads):
            cols = slice(h * HD, (h + 1) * HD)
            raw = acc[at_v, rollout_rows(x), cols] + pin[at_v, :, cols].astype(f32)
            raw = raw + lent_add(1, cols)
            value = jnp.where(live, raw, 0.0).astype(bf16)
            vbuf[:, cols] = value
            vext[h, :, :HD] = value
            vext[h, :, HD:] = jnp.where(live, 1.0, 0.0).astype(bf16)

    def share(j, parity):
        ref = att.at[parity, :, pl.ds(j * kw, kw)]
        return remote(ref, ref, asend.at[j], arecv.at[j], partner, mp)

    def attend(j):
        swap(at_q[j]).wait_recv()
        for i in range(kv_heads):
            h = j * kv_heads + i
            kv = h * kv_heads // q_heads
            cols, kcols = slice(i * HD, (i + 1) * HD), slice(kv * HD, (kv + 1) * HD)
            for r in range(n_mp):
                span, seen = slice(r * local_len, (r + 1) * local_len), (r + 1) * local_len
                raw = acc[at_q[j], rows_of(x, r), cols] + pin[at_q[j], span, cols].astype(f32)
                query = (rotated(raw, span) * 144.0 ** (-0.5)).astype(bf16)
                score = lax.dot_general(
                    query, kbuf[:seen, kcols], (((1,), (1,)), ((), ())),
                    preferred_element_type=f32,
                )
                row = lax.broadcasted_iota(jnp.int32, score.shape, 0) + r * local_len
                col = lax.broadcasted_iota(jnp.int32, score.shape, 1)
                expo = jnp.exp2(jnp.tanh(score * (1.0 / 50.0)) * (50.0 * np.log2(np.e)))
                expo = jnp.where(col <= row, expo, 0.0).astype(bf16)
                both = jnp.dot(expo, vext[kv, :seen, :], preferred_element_type=f32)
                att[x, span, h * HD : (h + 1) * HD] = (both[:, :HD] / both[:, HD:]).astype(bf16)
        share(j, x).start()

    relays(0, 1, 2)
    arrived(1 - x, mp).wait_recv()
    spread(1 - x)

    @pl.when(ends)
    def _():
        lend(1 - x).start()

    for load in load_w[2:] + [load_o]:
        load.wait()
    send_own(2)

    @pl.when(ends)
    def _():
        for c in range(3, nc + ns):
            send_own(c)

    pass_on(x)

    @pl.when(helps)
    def _():
        lent_spread(x)

    relays(0, 2, nz)
    relays(1, 1, 2)
    @pl.when(middle)
    def _():
        for c in range(3, nc):
            send_own(c)

    early = {0, ns - 1}
    for s in sorted(early):
        send_own_out(nc + s, z == 1, z == nz - 2)

    @pl.when(helps)
    def _():
        lent_spread(1 - x)

    pass_on(1 - x)
    for parity in (x, 1 - x):
        for step in range(pairs):
            arrived(parity, lax.rem(mate + 2 * step, n_mp)).wait_recv()
    compute(0)

    @pl.when(helps)
    def _():
        lent_pass(x)

    relays(1, 2, nz)
    relays(2, 1, 2)
    compute(1)

    @pl.when(helps)
    def _():
        lent_pass(1 - x)
        for parity in (x, 1 - x):
            for step in range(pairs):
                lent_wait(parity, lax.rem(mate + 2 * step, n_mp))
        lent_compute(0)

    for c in range(3, nc):
        relays(c, 1, 2)
    for load in load_r:
        load.wait()
    for t in range(width // LANES):
        pgain[:, t * LANES : (t + 1) * LANES] = pgain_t[t : t + 1, :]
    relays(2, 2, nz)

    @pl.when(helps)
    def _():
        lent_compute(1)

    compute(2)

    @pl.when(helps)
    def _():
        lent_finish(0)

    for c in range(3, nc):
        relays(c, 2, nz)
        compute(c)

    @pl.when(helps)
    def _():
        lent_finish(1)

    for s in range(ns):
        sent_out = s in early
        send_own_out(nc + s, z != 1 if sent_out else True, z != nz - 2 if sent_out else True)

    keys_done()
    values_done()
    for j in range(nq - 1):
        attend(j)

    def hand(s, zk, role, parity):
        return remote(
            psend[s].at[zk, parity, 1 - side], inbox[s].at[zk, parity],
            hsend.at[s], hrecv.at[s, zk, role], me, mate,
        )

    def far(s, zk, role, parity, step):
        target = lax.rem(mp + 2 * step, n_mp)
        return remote(
            psend[s].at[zk, parity, side, target // 2], precv[s].at[zk, parity, step - 1],
            fsend.at[s], frecv.at[s, zk, role, step - 1], me, target,
        )

    def back(s, zk, parity):
        return remote(
            xout[s].at[zk], yall[s].at[parity, zk], csend.at[s], crecv.at[s], partner, mp
        )

    def parity_of(role):
        return x if role == OWN else 1 - x

    def produce(s, zk, role):
        start, size = pieces[s]
        parity = parity_of(role)
        part = lax.dot_general(
            att[parity], obuf[zk, start : start + size, :], (((1,), (1,)), ((), ())),
            preferred_element_type=f32,
        ).astype(bf16)
        for p in range(n_mp):
            psend[s][zk, parity, p % 2, p // 2] = part[p * local_len : (p + 1) * local_len]
        hand(s, zk, role, parity).start()

    def combine(s, zk, role):
        parity = parity_of(role)
        hand(s, zk, role, parity).wait_recv()
        for step in range(1, pairs):
            q = lax.rem(mp + 2 * step, n_mp) // 2
            both = psend[s][zk, parity, side, q].astype(f32) + inbox[s][zk, parity, q].astype(f32)
            psend[s][zk, parity, side, q] = both.astype(bf16)
            far(s, zk, role, parity, step).start()

    def measure(value):
        value = value.astype(f32)
        sq[...] += jnp.sum(value * value, axis=-1, keepdims=True)

    def settle(s, zk, role):
        parity = parity_of(role)
        value = psend[s][zk, parity, side, slot].astype(f32)
        value = value + inbox[s][zk, parity, slot].astype(f32)
        for step in range(1, pairs):
            far(s, zk, role, parity, step).wait_recv()
            value = value + precv[s][zk, parity, step - 1].astype(f32)
        value = value.astype(bf16)
        if role == OWN:
            yall[s][x, zk] = value
            measure(value)
        else:
            xout[s][zk] = value
            back(s, zk, x).start()

    def around(k, act):
        def body(way, carry):
            zk = z + k * (2 * way - 1)

            @pl.when((zk >= 0) & (zk < nz) & ((way == 0) | (k > 0)))
            def _():
                act(zk)

            return carry

        lax.fori_loop(0, 2, body, 0)

    def near(act):
        def body(k, carry):
            around(k, act)
            return carry

        lax.fori_loop(0, min(2, nz), body, 0)

    attend(nq - 1)
    sq[...] = jnp.zeros_like(sq)
    for s in range(ns):
        produce(s, z, OWN)
    for s in range(ns):
        relays(nc + s, 1, 2)
        combine(s, z, OWN)
    for s in range(ns):
        around(1, functools.partial(produce, s, role=OWN))
    for s in range(ns):
        around(1, functools.partial(combine, s, role=OWN))
    for j in range(nq):
        share(j, 1 - x).wait_recv()
    for s in range(ns):
        near(functools.partial(produce, s, role=OTHER))
    for s in range(ns):
        near(functools.partial(combine, s, role=OTHER))

    def settle_near():
        for role in (OTHER, OWN):
            for s in range(ns):
                near(functools.partial(settle, s, role=role))

    def settle_at(s, k):
        def both(zk):
            for role in (OTHER, OWN):
                settle(s, zk, role)

        around(k, both)

    def late(k, carry):
        for s in range(ns):
            relay(nc + s, k)

            def make(zk, s=s):
                for role in (OTHER, OWN):
                    produce(s, zk, role)

            def join(zk, s=s):
                for role in (OTHER, OWN):
                    combine(s, zk, role)

            around(k, make)
            around(k, join)
            if s == 0:
                @pl.when(k == 3)
                def _():
                    settle_near()

            @pl.when(k > 2)
            def _():
                settle_at(s, k - 1)

        return carry

    lax.fori_loop(2, nz, late, 0)
    if nz < 4:
        settle_near()
    if nz > 2:
        for s in range(ns):
            settle_at(s, nz - 1)

    for s in range(ns):
        remote(xout[s], yall[s].at[1 - x], csend.at[s], crecv.at[s], partner, mp).wait_recv()

    def collect(zk, carry):
        for s in range(ns):
            measure(yall[s][1 - x, zk])
        return carry

    lax.fori_loop(0, nz, collect, 0)

    scale = lax.rsqrt(sq[...] / width + 1e-06)
    for block in range(n_dp):
        for s, (start, size) in enumerate(pieces):
            span = slice(block * fcols + start, block * fcols + start + size)
            own = lax.broadcasted_iota(jnp.int32, (local_len, size), 0) + mp * local_len < length
            post = yall[s][block % 2, block // 2].astype(f32) * scale * pgain[:, span]
            mbuf[:, span] = jnp.where(own, hid[:, span].astype(f32) + post, 0.0).astype(bf16)

    def sent(ref, sem):
        remote(ref, ref, sem, sem, partner, mp).wait_send()

    def drain_items(origin, carry):
        for way, mine in ((UP, origin <= z), (DOWN, origin >= z)):
            @pl.when(mine & sends(nc, origin, way))
            def _():
                sent(obuf.at[pl.ds(0, 2)], zsend.at[0, way, origin])

            @pl.when(mine & sends(at_k, origin, way))
            def _():
                sent(wbuf.at[pl.ds(at_k, 2), 0, pl.ds(0, rows_each)], zsend.at[1, way, origin])

        return carry

    lax.fori_loop(0, nz, drain_items, 0)
    for s in range(ns):
        sent(psend[s].at[:, :, 0], hsend.at[s])
        if pairs > 1:
            sent(precv[s], fsend.at[s])
        sent(xout[s], csend.at[s])
    across().wait_send()
    for parity in (x, 1 - x):
        for step in range(1, pairs):
            to_far(parity, step).wait_send()
        for step in range(pairs):
            to_mate(parity, lax.rem(mp + 2 * step, n_mp)).wait_send()
    for c in range(nc):
        swap(c).wait_send()

    @pl.when(ends)
    def _():
        for parity in range(2):
            lend(parity).wait_send()

    @pl.when(helps)
    def _():
        for parity in (x, 1 - x):
            for step in range(1, pairs):
                lent_far(parity, step).wait_send()
            for step in range(pairs):
                lent_mate(parity, lax.rem(mp + 2 * step, n_mp)).wait_send()
        for i in range(len(lent)):
            lent_swap(i).wait_send()
            lent_return(i).wait_send()

    for j in range(nq):
        share(j, x).wait_send()


def local(n_dp, n_mp, hidden, lengths, norm_gain, w_query, w_key, w_value, w_out, post_gain):
    _, local_len, width = hidden.shape
    maxlen = local_len * n_mp
    rows, qw = w_query.shape
    kw = w_key.shape[1]
    orows, fcols = w_out.shape
    nz, pairs = n_dp // 2, n_mp // 2
    far = max(1, pairs - 1)
    nq = qw // kw
    nc = 2 + nq
    pieces = cut(fcols)
    ns = len(pieces)
    cosine, sine = tables(maxlen)
    anywhere = pl.BlockSpec(memory_space=pl.ANY)
    bf16, f32 = jnp.bfloat16, jnp.float32
    dma = pltpu.SemaphoreType.DMA
    tiles = (width // LANES, LANES)

    def per_piece(*lead):
        return [pltpu.VMEM((*lead, local_len, size), bf16) for _, size in pieces]

    mixed, keys, values = pl.pallas_call(
        functools.partial(kernel, n_dp, n_mp, pieces),
        out_shape=(
            pltpu.VMEM((local_len, width), bf16),
            pltpu.VMEM((maxlen, kw), bf16),
            pltpu.VMEM((maxlen, kw), bf16),
        ),
        in_specs=[pl.BlockSpec(memory_space=pltpu.SMEM)] + [anywhere] * 9,
        out_specs=(pl.BlockSpec(memory_space=pltpu.VMEM),) * 3,
        scratch_shapes=[
            pltpu.VMEM((local_len, width), bf16),
            pltpu.VMEM(tiles, f32),
            pltpu.VMEM(tiles, f32),
            pltpu.VMEM((1, width), f32),
            pltpu.VMEM((1, width), f32),
            pltpu.VMEM((maxlen, HD), f32),
            pltpu.VMEM((maxlen, HD), f32),
            pltpu.VMEM((nc, 2, nz // 2 * rows, kw), bf16),
            pltpu.VMEM((nz, fcols, orows), bf16),
            pltpu.VMEM((2, 2 * maxlen + local_len, nz // 2 * rows), bf16),
            pltpu.VMEM((nc, 2 * maxlen, kw), f32),
            pltpu.VMEM((nc, maxlen, kw), bf16),
            pltpu.VMEM((nc, maxlen, kw), bf16),
            pltpu.VMEM((kw // HD, maxlen, 2 * HD), bf16),
            pltpu.VMEM((2, maxlen, qw), bf16),
            pltpu.VMEM((local_len, 1), f32),
            pltpu.VMEM((2 * maxlen, nz // 2 * rows), bf16),
            pltpu.VMEM((2, 2 * maxlen, kw), f32),
            pltpu.VMEM((2, maxlen, kw), bf16),
            pltpu.VMEM((2, maxlen, kw), bf16),
            pltpu.VMEM((2, maxlen, kw), bf16),
            pltpu.VMEM((2, maxlen, kw), bf16),
            *per_piece(nz, 2, 2, pairs),
            *per_piece(nz, 2, pairs),
            *per_piece(nz, 2, far),
            *per_piece(nz),
            *per_piece(2, nz),
            dma((nc + 6,)),
            dma((2, 2, nz)),
            dma((nc + ns, nz)),
            dma((1,)),
            dma((2, pairs)),
            dma((2, far)),
            dma((2, n_mp)),
            dma((nc,)),
            dma((nc,)),
            dma((nq,)),
            dma((nq,)),
            dma((ns,)),
            dma((ns, nz, 2)),
            dma((ns,)),
            dma((ns, nz, 2, far)),
            dma((ns,)),
            dma((ns,)),
            dma((2,)),
            dma((2, pairs)),
            dma((2, far)),
            dma((2, n_mp)),
            dma((2,)),
            dma((2,)),
            dma((2,)),
            dma((2,)),
        ],
        compiler_params=pltpu.CompilerParams(
            collective_id=0, has_side_effects=True, vmem_limit_bytes=60 * 1024 * 1024
        ),
    )(
        lengths,
        hidden[0],
        norm_gain.reshape(tiles),
        w_query,
        w_key,
        w_value,
        w_out.T,
        post_gain.reshape(tiles),
        jnp.asarray(cosine),
        jnp.asarray(sine),
    )
    return mixed[None], keys[None], values[None]


def solution(mesh):
    return jax.shard_map(
        functools.partial(local, mesh.shape["dp"], mesh.shape["mp"]),
        mesh=mesh,
        in_specs=(
            P("dp", "mp", None),
            P("dp"),
            P(),
            P("dp", "mp"),
            P("dp", "mp"),
            P("dp", "mp"),
            P("mp", "dp"),
            P(),
        ),
        out_specs=(P("dp", "mp", None), P("dp", None, "mp"), P("dp", None, "mp")),
        check_vma=False,
    )
```

```python
import functools

import jax
import jax.numpy as jnp
import numpy as np
from jax import lax
from jax.experimental import pallas as pl
from jax.experimental.pallas import tpu as pltpu
from jax.sharding import PartitionSpec as P

HD = 128
LANES = 128
MESH = pl.DeviceIdType.MESH
UP, DOWN = 0, 1
OWN, OTHER = 0, 1


def tables(maxlen):
    half = HD // 2
    freqs = 10000.0 ** (-np.arange(half, dtype=np.float64) / half)
    angles = np.arange(maxlen, dtype=np.float64)[:, None] * freqs[None, :]
    cosine, sine = np.cos(angles), np.sin(angles)
    return (
        np.concatenate([cosine, cosine], axis=1).astype(np.float32),
        np.concatenate([-sine, sine], axis=1).astype(np.float32),
    )


def cut(rows):
    pieces, start = [], 0
    while start < rows:
        size = min(256, rows - start)
        pieces.append((start, size))
        start += size
    return pieces


def packed(size):
    return 2 * size <= LANES


def kernel(
    n_dp, n_mp, pieces,
    len_in, hid_in, ngain_in, wq, wk, wv, wo, pgain_in, cos_in, sin_in,
    mbuf, kbuf, vbuf,
    *scratch,
):
    ns = len(pieces)
    (
        hid, ngain_t, pgain_t, ngain, pgain, cos_ref, sin_ref,
        wbuf, obuf, nbuf, acc, pout, pin, vext, att, sq,
        hrows, hacc, hpout, hpin, hsum, epin, len_ref,
    ) = scratch[:23]
    rest = scratch[23:]
    psend, inbox, precv, xout, yall = (rest[i * ns : (i + 1) * ns] for i in range(5))
    (
        load_sem, zsend, zrecv, xsend, xmate, xfar, xrecv, qsend, qrecv, asend, arecv,
        hsend, hrecv, fsend, frecv, csend, crecv,
        lsend, lmate, lfar, lrecv, bsend, brecv, esend, erecv,
    ) = rest[5 * ns :]

    nz = n_dp // 2
    pairs = n_mp // 2
    me, mp = lax.axis_index("dp"), lax.axis_index("mp")
    z, x = me // 2, me % 2
    side, slot = mp % 2, mp // 2
    partner = me + 1 - 2 * x
    mate = mp + 1 - 2 * side
    local_len, width = hid.shape
    maxlen = local_len * n_mp
    fcols = width // n_dp
    rows_each = wq.shape[0]
    qw, kw = wq.shape[1], wk.shape[1]
    nq = qw // kw
    nc = 2 + nq
    at_k, at_v = 1, 2
    at_q = [0] + list(range(3, nc))
    lent = (at_k, at_v)
    half = nz // 2
    q_heads, kv_heads = qw // HD, kw // HD
    can_up, can_down = z < nz - 1, z > 0
    middle = can_up & can_down
    ends = jnp.logical_not(middle)
    helps = (z == 1) | (z == nz - 2)
    far_half = jnp.where((z == 0) | (z == 1), 1, 0)
    inward = jnp.where(z == 0, me + 2, me - 2)
    outward = jnp.where(z == 1, me - 2, me + 2)
    f32, bf16 = jnp.float32, jnp.bfloat16

    def remote(src, dst, send, recv, dp_index, mp_index):
        return pltpu.make_async_remote_copy(
            src_ref=src, dst_ref=dst, send_sem=send, recv_sem=recv,
            device_id=(dp_index, mp_index), device_id_type=MESH,
        )

    def item(c, origin):
        if c < nc:
            first = pl.multiple_of(origin % half * rows_each, rows_each)
            return wbuf.at[c, origin // half, pl.ds(first, rows_each)]
        start, size = pieces[c - nc]
        return obuf.at[origin, pl.ds(start, size)]

    sources = [None] * nc
    sources[at_k], sources[at_v] = wk, wv
    for j, c in enumerate(at_q):
        sources[c] = wq.at[:, pl.ds(j * kw, kw)]
    load_w = [
        pltpu.make_async_copy(source, item(c, z), load_sem.at[c])
        for c, source in enumerate(sources)
    ]
    load_o = pltpu.make_async_copy(wo, obuf.at[z], load_sem.at[nc])
    load_x = [
        pltpu.make_async_copy(hid_in, hid, load_sem.at[nc + 1]),
        pltpu.make_async_copy(ngain_in, ngain_t, load_sem.at[nc + 2]),
    ]
    load_r = [
        pltpu.make_async_copy(pgain_in, pgain_t, load_sem.at[nc + 3]),
        pltpu.make_async_copy(cos_in, cos_ref, load_sem.at[nc + 4]),
        pltpu.make_async_copy(sin_in, sin_ref, load_sem.at[nc + 5]),
        pltpu.make_async_copy(len_in, len_ref, load_sem.at[nc + 6]),
    ]
    for load in load_w[:1] + load_x + load_w[1:] + [load_o] + load_r:
        load.start()

    barrier = pltpu.get_barrier_semaphore()

    def greet(dp_index, mp_index):
        pl.semaphore_signal(barrier, inc=1, device_id=(dp_index, mp_index), device_id_type=MESH)

    greet(partner, mp)
    for step in range(1, n_mp):
        greet(me, lax.rem(mp + step, n_mp))

    @pl.when(can_up)
    def _():
        greet(me + 2, mp)

    @pl.when(can_down)
    def _():
        greet(me - 2, mp)

    pl.semaphore_wait(
        barrier, n_mp + jnp.where(can_up, 1, 0) + jnp.where(can_down, 1, 0)
    )

    def copy(c, origin, way):
        ref = item(c, origin)
        return remote(
            ref, ref, zsend.at[1 if c in lent else 0, way, origin], zrecv.at[c, origin],
            (me + 2, me - 2)[way], mp,
        )

    def sends(c, origin, way):
        if way == UP:
            skip, able = (z + 1 == nz - 1) & (origin < half), can_up
        else:
            skip, able = (z - 1 == 0) & (origin >= half), can_down
        return able & jnp.logical_not(skip) if c in lent else able

    def gets(c, origin):
        if c not in lent:
            return (origin >= 0) & (origin < nz)
        low, high = jnp.where(z == nz - 1, half, 0), jnp.where(z == 0, half, nz)
        return (origin >= low) & (origin < high)

    def send(c, origin, way):
        @pl.when(sends(c, origin, way))
        def _():
            copy(c, origin, way).start()

    def send_own(c):
        send(c, z, UP)
        send(c, z, DOWN)

    def send_own_out(c, down, up):
        @pl.when(down & middle)
        def _():
            copy(c, z, DOWN).start()

        @pl.when(up & middle)
        def _():
            copy(c, z, UP).start()

    def relay(c, k):
        for origin, way in ((z - k, UP), (z + k, DOWN)):
            @pl.when(gets(c, origin))
            def _():
                copy(c, origin, way).wait_recv()
                send(c, origin, way)

    def relays(c, first, last):
        def body(k, carry):
            relay(c, k)
            return carry

        lax.fori_loop(first, last, body, 0)

    def rows_of(parity, block):
        return pl.ds(pl.multiple_of(parity * maxlen + block * local_len, local_len), local_len)

    def region(parity, block):
        return nbuf.at[:, rows_of(parity, block), :]

    def across():
        return remote(
            nbuf.at[:, pl.ds(2 * maxlen, local_len), :], region(x, mp),
            xsend.at[0], xrecv.at[x, mp], partner, mp,
        )

    def to_mate(parity, block):
        return remote(
            region(parity, block), region(parity, block),
            xmate.at[parity, block // 2], xrecv.at[parity, block], me, mate,
        )

    def to_far(parity, step):
        return remote(
            region(parity, mp), region(parity, mp),
            xfar.at[parity, step - 1], xrecv.at[parity, mp], me, lax.rem(mp + 2 * step, n_mp),
        )

    def arrived(parity, block):
        return remote(
            region(parity, block), region(parity, block),
            xsend.at[0], xrecv.at[parity, block], me, mate,
        )

    def spread(parity):
        for step in range(1, pairs):
            to_far(parity, step).start()
        to_mate(parity, mp).start()

    def pass_on(parity):
        for step in range(1, pairs):
            block = lax.rem(mp + 2 * step, n_mp)
            arrived(parity, block).wait_recv()
            to_mate(parity, block).start()

    def lend(parity):
        return remote(
            nbuf.at[far_half, rows_of(parity, mp), :],
            hrows.at[rows_of(parity, mp), :],
            lsend.at[parity], lrecv.at[parity, mp], inward, mp,
        )

    def lent_to(parity, block, dst, send_sem):
        ref = hrows.at[rows_of(parity, block), :]
        return remote(ref, ref, send_sem, lrecv.at[parity, block], me, dst)

    def lent_mate(parity, block):
        return lent_to(parity, block, mate, lmate.at[parity, block // 2])

    def lent_far(parity, step):
        return lent_to(parity, mp, lax.rem(mp + 2 * step, n_mp), lfar.at[parity, step - 1])

    def lent_wait(parity, block):
        lent_to(parity, block, mate, lsend.at[parity]).wait_recv()

    def lent_spread(parity):
        lent_wait(parity, mp)
        for step in range(1, pairs):
            lent_far(parity, step).start()
        lent_mate(parity, mp).start()

    def lent_pass(parity):
        for step in range(1, pairs):
            block = lax.rem(mp + 2 * step, n_mp)
            lent_wait(parity, block)
            lent_mate(parity, block).start()

    load_w[0].wait()
    send_own(0)
    for load in load_x:
        load.wait()
    for t in range(width // LANES):
        ngain[:, t * LANES : (t + 1) * LANES] = ngain_t[t : t + 1, :]
    total = jnp.zeros((local_len, LANES), f32)
    for t in range(width // LANES):
        rows = hid[:, t * LANES : (t + 1) * LANES].astype(f32)
        total = total + rows * rows
    scale = lax.rsqrt(jnp.sum(total, axis=-1, keepdims=True) / width + 1e-06)
    for block in range(n_dp):
        span = slice(block * fcols, (block + 1) * fcols)
        rows = hid[:, span].astype(f32)
        first = jnp.where(x == block % 2, x * maxlen + mp * local_len, 2 * maxlen)
        k = block // 2
        cols = slice(k % half * fcols, (k % half + 1) * fcols)
        nbuf[k // half, pl.ds(pl.multiple_of(first, local_len), local_len), cols] = (
            rows * scale * ngain[:, span]
        ).astype(bf16)
    across().start()
    spread(x)

    @pl.when(ends)
    def _():
        lend(x).start()

    load_w[1].wait()
    send_own(1)
    acc[...] = jnp.zeros_like(acc)

    @pl.when(middle)
    def _():
        epin[...] = jnp.zeros_like(epin)

    def rollout_rows(parity):
        return pl.ds(pl.multiple_of(parity * maxlen, maxlen), maxlen)

    def swap(c):
        return remote(pout.at[c], pin.at[c], qsend.at[c], qrecv.at[c], partner, mp)

    def compute(c):
        first, last = 0, 2
        if c in lent:
            first, last = jnp.where(z == nz - 1, 1, 0), jnp.where(z == 0, 1, 2)

        def contract(parity):
            rows = rollout_rows(parity)

            def body(k, carry):
                acc[c, rows, :] += jnp.dot(
                    nbuf[k, rows, :], wbuf[c, k], preferred_element_type=f32
                )
                return carry

            lax.fori_loop(first, last, body, 0)

        contract(1 - x)
        pout[c] = acc[c, rollout_rows(1 - x), :].astype(bf16)
        swap(c).start()
        contract(x)

    def lent_swap(i):
        return remote(hpout.at[i], hpin.at[i], bsend.at[i], brecv.at[i], partner, mp)

    def lent_return(i):
        return remote(hsum.at[i], epin.at[i], esend.at[i], erecv.at[i], outward, mp)

    def lent_compute(i):
        def contract(parity):
            rows = rollout_rows(parity)

            hacc[i, rows, :] = jnp.dot(
                hrows[rows, :], wbuf[lent[i], far_half], preferred_element_type=f32
            )

        contract(1 - x)
        hpout[i] = hacc[i, rollout_rows(1 - x), :].astype(bf16)
        lent_swap(i).start()
        contract(x)

    def lent_finish(i):
        lent_swap(i).wait_recv()
        hsum[i] = (hacc[i, rollout_rows(x), :] + hpin[i].astype(f32)).astype(bf16)
        lent_return(i).start()

    def lent_add(i, cols):
        return epin[i, :, cols].astype(f32)

    def lent_ready(i):
        @pl.when(ends)
        def _():
            lent_return(i).wait_recv()

    def rotated(block, span):
        return block * cos_ref[span, :] + pltpu.roll(block, HD // 2, 1) * sin_ref[span, :]

    everything = slice(0, maxlen)

    def keys_done():
        swap(at_k).wait_recv()
        lent_ready(0)
        for h in range(kv_heads):
            cols = slice(h * HD, (h + 1) * HD)
            raw = acc[at_k, rollout_rows(x), cols] + pin[at_k, :, cols].astype(f32)
            raw = raw + lent_add(0, cols)
            kbuf[:, cols] = jnp.where(live, rotated(raw, everything), 0.0).astype(bf16)

    def values_done():
        swap(at_v).wait_recv()
        lent_ready(1)
        for h in range(kv_heads):
            cols = slice(h * HD, (h + 1) * HD)
            raw = acc[at_v, rollout_rows(x), cols] + pin[at_v, :, cols].astype(f32)
            raw = raw + lent_add(1, cols)
            value = jnp.where(live, raw, 0.0).astype(bf16)
            vbuf[:, cols] = value
            vext[h, :, :HD] = value
            vext[h, :, HD:] = jnp.where(live, 1.0, 0.0).astype(bf16)

    def share(j, parity):
        ref = att.at[parity, :, pl.ds(j * kw, kw)]
        return remote(ref, ref, asend.at[j], arecv.at[j], partner, mp)

    def attend(j):
        swap(at_q[j]).wait_recv()
        for i in range(kv_heads):
            h = j * kv_heads + i
            kv = h * kv_heads // q_heads
            cols, kcols = slice(i * HD, (i + 1) * HD), slice(kv * HD, (kv + 1) * HD)
            for r in range(n_mp):
                span, seen = slice(r * local_len, (r + 1) * local_len), (r + 1) * local_len
                raw = acc[at_q[j], rows_of(x, r), cols] + pin[at_q[j], span, cols].astype(f32)
                query = (rotated(raw, span) * 144.0 ** (-0.5)).astype(bf16)
                score = lax.dot_general(
                    query, kbuf[:seen, kcols], (((1,), (1,)), ((), ())),
                    preferred_element_type=f32,
                )
                row = lax.broadcasted_iota(jnp.int32, score.shape, 0) + r * local_len
                col = lax.broadcasted_iota(jnp.int32, score.shape, 1)
                expo = jnp.exp2(jnp.tanh(score * (1.0 / 50.0)) * (50.0 * np.log2(np.e)))
                expo = jnp.where(col <= row, expo, 0.0).astype(bf16)
                both = jnp.dot(expo, vext[kv, :seen, :], preferred_element_type=f32)
                att[x, span, h * HD : (h + 1) * HD] = (both[:, :HD] / both[:, HD:]).astype(bf16)
        share(j, x).start()

    relays(0, 1, 2)
    arrived(1 - x, mp).wait_recv()
    spread(1 - x)

    @pl.when(ends)
    def _():
        lend(1 - x).start()

    for load in load_w[2:] + [load_o]:
        load.wait()
    send_own(2)

    @pl.when(ends)
    def _():
        for c in range(3, nc + ns):
            send_own(c)

    pass_on(x)

    @pl.when(helps)
    def _():
        lent_spread(x)

    relays(0, 2, nz)
    relays(1, 1, 2)
    @pl.when(middle)
    def _():
        for c in range(3, nc):
            send_own(c)

    early = {0, ns - 1}
    for s in sorted(early):
        send_own_out(nc + s, z == 1, z == nz - 2)

    @pl.when(helps)
    def _():
        lent_spread(1 - x)

    pass_on(1 - x)
    for parity in (x, 1 - x):
        for step in range(pairs):
            arrived(parity, lax.rem(mate + 2 * step, n_mp)).wait_recv()
    compute(0)

    @pl.when(helps)
    def _():
        lent_pass(x)

    relays(1, 2, nz)
    relays(2, 1, 2)
    compute(1)

    @pl.when(helps)
    def _():
        lent_pass(1 - x)
        for parity in (x, 1 - x):
            for step in range(pairs):
                lent_wait(parity, lax.rem(mate + 2 * step, n_mp))
        lent_compute(0)

    for c in range(3, nc):
        relays(c, 1, 2)
    for load in load_r:
        load.wait()
    length = len_ref[0]
    live = lax.broadcasted_iota(jnp.int32, (maxlen, HD), 0) < length
    for t in range(width // LANES):
        pgain[:, t * LANES : (t + 1) * LANES] = pgain_t[t : t + 1, :]
    relays(2, 2, nz)

    @pl.when(helps)
    def _():
        lent_compute(1)

    compute(2)

    @pl.when(helps)
    def _():
        lent_finish(0)

    for c in range(3, nc):
        relays(c, 2, nz)
        compute(c)

    @pl.when(helps)
    def _():
        lent_finish(1)

    for s in range(ns):
        sent_out = s in early
        send_own_out(nc + s, z != 1 if sent_out else True, z != nz - 2 if sent_out else True)

    keys_done()
    values_done()
    for j in range(nq - 1):
        attend(j)

    def hand(s, zk, role, parity):
        return remote(
            psend[s].at[zk, parity, 1 - side], inbox[s].at[zk, parity],
            hsend.at[s], hrecv.at[s, zk, role], me, mate,
        )

    def far(s, zk, role, parity, step):
        target = lax.rem(mp + 2 * step, n_mp)
        return remote(
            psend[s].at[zk, parity, side, target // 2], precv[s].at[zk, parity, step - 1],
            fsend.at[s], frecv.at[s, zk, role, step - 1], me, target,
        )

    def back(s, zk, parity):
        return remote(
            xout[s].at[zk], yall[s].at[parity, zk], csend.at[s], crecv.at[s], partner, mp
        )

    def roles_of(s):
        return (OTHER,) if packed(pieces[s][1]) else (OTHER, OWN)

    def parity_of(role):
        return x if role == OWN else 1 - x

    def lead_of(s, role):
        return 0 if packed(pieces[s][1]) else parity_of(role)

    def produce(s, zk, role):
        start, size = pieces[s]
        lead = lead_of(s, role)

        def project(parity, weights):
            return lax.dot_general(
                att[parity], weights, (((1,), (1,)), ((), ())), preferred_element_type=f32
            )

        weights = obuf[zk, start : start + size, :]
        if packed(size):
            blank = jnp.zeros_like(weights)
            part = project(0, jnp.concatenate([weights, blank], axis=0))
            part = part + project(1, jnp.concatenate([blank, weights], axis=0))
        else:
            part = project(lead, weights)
        part = part.astype(bf16)
        for p in range(n_mp):
            psend[s][zk, lead, p % 2, p // 2] = part[p * local_len : (p + 1) * local_len]
        hand(s, zk, role, lead).start()

    def combine(s, zk, role):
        parity = lead_of(s, role)
        hand(s, zk, role, parity).wait_recv()
        for step in range(1, pairs):
            q = lax.rem(mp + 2 * step, n_mp) // 2
            both = psend[s][zk, parity, side, q].astype(f32) + inbox[s][zk, parity, q].astype(f32)
            psend[s][zk, parity, side, q] = both.astype(bf16)
            far(s, zk, role, parity, step).start()

    def measure(value):
        value = value.astype(f32)
        sq[...] += jnp.sum(value * value, axis=-1, keepdims=True)

    def settle(s, zk, role):
        parity = lead_of(s, role)
        value = psend[s][zk, parity, side, slot].astype(f32)
        value = value + inbox[s][zk, parity, slot].astype(f32)
        for step in range(1, pairs):
            far(s, zk, role, parity, step).wait_recv()
            value = value + precv[s][zk, parity, step - 1].astype(f32)
        size = pieces[s][1]
        if packed(size):
            swapped = pltpu.roll(value, size, 1)
            ours = jnp.where(x == 0, value, swapped)[:, :size].astype(bf16)
            theirs = jnp.where(x == 0, swapped, value)[:, :size].astype(bf16)
            xout[s][zk] = theirs
            back(s, zk, x).start()
            yall[s][x, zk] = ours
            measure(ours)
            return
        value = value.astype(bf16)
        if role == OWN:
            yall[s][x, zk] = value
            measure(value)
        else:
            xout[s][zk] = value
            back(s, zk, x).start()

    def around(k, act):
        def body(way, carry):
            zk = z + k * (2 * way - 1)

            @pl.when((zk >= 0) & (zk < nz) & ((way == 0) | (k > 0)))
            def _():
                act(zk)

            return carry

        lax.fori_loop(0, 2, body, 0)

    def near(act):
        def body(k, carry):
            around(k, act)
            return carry

        lax.fori_loop(0, min(2, nz), body, 0)

    attend(nq - 1)
    sq[...] = jnp.zeros_like(sq)
    single = [s for s in range(ns) if OWN in roles_of(s)]
    for s in single:
        produce(s, z, OWN)
    for s in range(ns):
        relays(nc + s, 1, 2)
        if s in single:
            combine(s, z, OWN)
    for s in single:
        around(1, functools.partial(produce, s, role=OWN))
    for s in single:
        around(1, functools.partial(combine, s, role=OWN))
    for j in range(nq):
        share(j, 1 - x).wait_recv()
    for s in range(ns):
        near(functools.partial(produce, s, role=OTHER))
    for s in range(ns):
        near(functools.partial(combine, s, role=OTHER))

    def settle_near():
        for role in (OTHER, OWN):
            for s in range(ns):
                if role in roles_of(s):
                    late_here = True if role == OWN or s == ns - 1 else middle

                    @pl.when(late_here)
                    def _():
                        near(functools.partial(settle, s, role=role))

    def settle_at(s, k):
        def both(zk):
            for role in roles_of(s):
                settle(s, zk, role)

        around(k, both)

    def late(k, carry):
        for s in range(ns):
            relay(nc + s, k)

            def make(zk, s=s):
                for role in roles_of(s):
                    produce(s, zk, role)

            def join(zk, s=s):
                for role in roles_of(s):
                    combine(s, zk, role)

            around(k, make)
            around(k, join)
            if s == 0:
                @pl.when(k == 3)
                def _():
                    settle_near()
            else:
                @pl.when((k == 2) & ends)
                def _():
                    near(functools.partial(settle, s - 1, role=OTHER))

            @pl.when(k > 2)
            def _():
                settle_at(s, k - 1)

        return carry

    lax.fori_loop(2, nz, late, 0)
    if nz < 4:
        settle_near()
    if nz > 2:
        for s in range(ns):
            settle_at(s, nz - 1)

    for s in range(ns):
        remote(xout[s], yall[s].at[1 - x], csend.at[s], crecv.at[s], partner, mp).wait_recv()

    def collect(zk, carry):
        for s in range(ns):
            measure(yall[s][1 - x, zk])
        return carry

    lax.fori_loop(0, nz, collect, 0)

    scale = lax.rsqrt(sq[...] / width + 1e-06)
    for block in range(n_dp):
        for s, (start, size) in enumerate(pieces):
            span = slice(block * fcols + start, block * fcols + start + size)
            own = lax.broadcasted_iota(jnp.int32, (local_len, size), 0) + mp * local_len < length
            post = yall[s][block % 2, block // 2].astype(f32) * scale * pgain[:, span]
            mbuf[:, span] = jnp.where(own, hid[:, span].astype(f32) + post, 0.0).astype(bf16)

    def sent(ref, sem):
        remote(ref, ref, sem, sem, partner, mp).wait_send()

    def drain_items(origin, carry):
        for way, mine in ((UP, origin <= z), (DOWN, origin >= z)):
            @pl.when(mine & sends(nc, origin, way))
            def _():
                sent(obuf.at[pl.ds(0, 2)], zsend.at[0, way, origin])

            @pl.when(mine & sends(at_k, origin, way))
            def _():
                sent(wbuf.at[pl.ds(at_k, 2), 0, pl.ds(0, rows_each)], zsend.at[1, way, origin])

        return carry

    lax.fori_loop(0, nz, drain_items, 0)
    for s in range(ns):
        sent(psend[s].at[:, :, 0], hsend.at[s])
        if pairs > 1:
            sent(precv[s], fsend.at[s])
        sent(xout[s], csend.at[s])
    across().wait_send()
    for parity in (x, 1 - x):
        for step in range(1, pairs):
            to_far(parity, step).wait_send()
        for step in range(pairs):
            to_mate(parity, lax.rem(mp + 2 * step, n_mp)).wait_send()
    for c in range(nc):
        swap(c).wait_send()

    @pl.when(ends)
    def _():
        for parity in range(2):
            lend(parity).wait_send()

    @pl.when(helps)
    def _():
        for parity in (x, 1 - x):
            for step in range(1, pairs):
                lent_far(parity, step).wait_send()
            for step in range(pairs):
                lent_mate(parity, lax.rem(mp + 2 * step, n_mp)).wait_send()
        for i in range(len(lent)):
            lent_swap(i).wait_send()
            lent_return(i).wait_send()

    for j in range(nq):
        share(j, x).wait_send()


def local(n_dp, n_mp, hidden, lengths, norm_gain, w_query, w_key, w_value, w_out, post_gain):
    _, local_len, width = hidden.shape
    maxlen = local_len * n_mp
    rows, qw = w_query.shape
    kw = w_key.shape[1]
    orows, fcols = w_out.shape
    nz, pairs = n_dp // 2, n_mp // 2
    far = max(1, pairs - 1)
    nq = qw // kw
    nc = 2 + nq
    pieces = cut(fcols)
    ns = len(pieces)
    cosine, sine = tables(maxlen)
    anywhere = pl.BlockSpec(memory_space=pl.ANY)
    bf16, f32 = jnp.bfloat16, jnp.float32
    dma = pltpu.SemaphoreType.DMA
    tiles = (width // LANES, LANES)

    def per_piece(*lead):
        return [pltpu.VMEM((*lead, local_len, size), bf16) for _, size in pieces]

    def per_sum(*rest):
        return [
            pltpu.VMEM((nz, 1 if packed(size) else 2, *rest, local_len, size * (1 + packed(size))), bf16)
            for _, size in pieces
        ]

    mixed, keys, values = pl.pallas_call(
        functools.partial(kernel, n_dp, n_mp, pieces),
        out_shape=(
            pltpu.VMEM((local_len, width), bf16),
            pltpu.VMEM((maxlen, kw), bf16),
            pltpu.VMEM((maxlen, kw), bf16),
        ),
        in_specs=[anywhere] * 10,
        out_specs=(pl.BlockSpec(memory_space=pltpu.VMEM),) * 3,
        scratch_shapes=[
            pltpu.VMEM((local_len, width), bf16),
            pltpu.VMEM(tiles, f32),
            pltpu.VMEM(tiles, f32),
            pltpu.VMEM((1, width), f32),
            pltpu.VMEM((1, width), f32),
            pltpu.VMEM((maxlen, HD), f32),
            pltpu.VMEM((maxlen, HD), f32),
            pltpu.VMEM((nc, 2, nz // 2 * rows, kw), bf16),
            pltpu.VMEM((nz, fcols, orows), bf16),
            pltpu.VMEM((2, 2 * maxlen + local_len, nz // 2 * rows), bf16),
            pltpu.VMEM((nc, 2 * maxlen, kw), f32),
            pltpu.VMEM((nc, maxlen, kw), bf16),
            pltpu.VMEM((nc, maxlen, kw), bf16),
            pltpu.VMEM((kw // HD, maxlen, 2 * HD), bf16),
            pltpu.VMEM((2, maxlen, qw), bf16),
            pltpu.VMEM((local_len, 1), f32),
            pltpu.VMEM((2 * maxlen, nz // 2 * rows), bf16),
            pltpu.VMEM((2, 2 * maxlen, kw), f32),
            pltpu.VMEM((2, maxlen, kw), bf16),
            pltpu.VMEM((2, maxlen, kw), bf16),
            pltpu.VMEM((2, maxlen, kw), bf16),
            pltpu.VMEM((2, maxlen, kw), bf16),
            pltpu.SMEM((1,), jnp.int32),
            *per_sum(2, pairs),
            *per_sum(pairs),
            *per_sum(far),
            *per_piece(nz),
            *per_piece(2, nz),
            dma((nc + 7,)),
            dma((2, 2, nz)),
            dma((nc + ns, nz)),
            dma((1,)),
            dma((2, pairs)),
            dma((2, far)),
            dma((2, n_mp)),
            dma((nc,)),
            dma((nc,)),
            dma((nq,)),
            dma((nq,)),
            dma((ns,)),
            dma((ns, nz, 2)),
            dma((ns,)),
            dma((ns, nz, 2, far)),
            dma((ns,)),
            dma((ns,)),
            dma((2,)),
            dma((2, pairs)),
            dma((2, far)),
            dma((2, n_mp)),
            dma((2,)),
            dma((2,)),
            dma((2,)),
            dma((2,)),
        ],
        compiler_params=pltpu.CompilerParams(
            collective_id=0, has_side_effects=True, vmem_limit_bytes=60 * 1024 * 1024
        ),
    )(
        lengths,
        hidden[0],
        norm_gain.reshape(tiles),
        w_query,
        w_key,
        w_value,
        w_out.T,
        post_gain.reshape(tiles),
        jnp.asarray(cosine),
        jnp.asarray(sine),
    )
    return mixed[None], keys[None], values[None]


def solution(mesh):
    return jax.shard_map(
        functools.partial(local, mesh.shape["dp"], mesh.shape["mp"]),
        mesh=mesh,
        in_specs=(
            P("dp", "mp", None),
            P("dp"),
            P(),
            P("dp", "mp"),
            P("dp", "mp"),
            P("dp", "mp"),
            P("mp", "dp"),
            P(),
        ),
        out_specs=(P("dp", "mp", None), P("dp", None, "mp"), P("dp", None, "mp")),
        check_vma=False,
    )
```

```python
import functools

import jax
import jax.numpy as jnp
import numpy as np
from jax import lax
from jax.experimental import pallas as pl
from jax.experimental.pallas import tpu as pltpu
from jax.sharding import PartitionSpec as P

HD = 128
LANES = 128
MESH = pl.DeviceIdType.MESH
UP, DOWN = 0, 1
OWN, OTHER = 0, 1


def tables(maxlen):
    half = HD // 2
    freqs = 10000.0 ** (-np.arange(half, dtype=np.float64) / half)
    angles = np.arange(maxlen, dtype=np.float64)[:, None] * freqs[None, :]
    cosine, sine = np.cos(angles), np.sin(angles)
    return (
        np.concatenate([cosine, cosine], axis=1).astype(np.float32),
        np.concatenate([-sine, sine], axis=1).astype(np.float32),
    )


def cut(rows):
    pieces, start = [], 0
    while start < rows:
        size = min(256, rows - start)
        pieces.append((start, size))
        start += size
    return pieces


def packed(size):
    return 2 * size <= LANES


def kernel(
    n_dp, n_mp, pieces,
    len_in, hid_in, ngain_in, wq, wk, wv, wo, pgain_in, cos_in, sin_in,
    mbuf, kbuf, vbuf,
    *scratch,
):
    ns = len(pieces)
    (
        hid, ngain_t, pgain_t, ngain, pgain, cos_ref, sin_ref,
        wbuf, obuf, nbuf, acc, pout, pin, vext, att, sq,
        hrows, hacc, hpout, hpin, hsum, epin, len_ref,
    ) = scratch[:23]
    rest = scratch[23:]
    psend, inbox, precv, xout, yall = (rest[i * ns : (i + 1) * ns] for i in range(5))
    (
        load_sem, zsend, zrecv, xsend, xmate, xfar, xrecv, qsend, qrecv, asend, arecv,
        hsend, hrecv, fsend, frecv, csend, crecv,
        lsend, lmate, lfar, lrecv, bsend, brecv, esend, erecv,
    ) = rest[5 * ns :]

    nz = n_dp // 2
    pairs = n_mp // 2
    me, mp = lax.axis_index("dp"), lax.axis_index("mp")
    z, x = me // 2, me % 2
    side, slot = mp % 2, mp // 2
    partner = me + 1 - 2 * x
    mate = mp + 1 - 2 * side
    local_len, width = hid.shape
    maxlen = local_len * n_mp
    fcols = width // n_dp
    rows_each = wq.shape[0]
    qw, kw = wq.shape[1], wk.shape[1]
    nq = qw // kw
    nc = 2 + nq
    at_k, at_v = 1, 2
    at_q = [0] + list(range(3, nc))
    lent = (at_k, at_v)
    half = nz // 2
    q_heads, kv_heads = qw // HD, kw // HD
    can_up, can_down = z < nz - 1, z > 0
    middle = can_up & can_down
    ends = jnp.logical_not(middle)
    helps = (z == 1) | (z == nz - 2)
    far_half = jnp.where((z == 0) | (z == 1), 1, 0)
    inward = jnp.where(z == 0, me + 2, me - 2)
    outward = jnp.where(z == 1, me - 2, me + 2)
    f32, bf16 = jnp.float32, jnp.bfloat16

    def remote(src, dst, send, recv, dp_index, mp_index):
        return pltpu.make_async_remote_copy(
            src_ref=src, dst_ref=dst, send_sem=send, recv_sem=recv,
            device_id=(dp_index, mp_index), device_id_type=MESH,
        )

    def item(c, origin):
        if c < nc:
            first = pl.multiple_of(origin % half * rows_each, rows_each)
            return wbuf.at[c, origin // half, pl.ds(first, rows_each)]
        start, size = pieces[c - nc]
        return obuf.at[origin, pl.ds(start, size)]

    sources = [None] * nc
    sources[at_k], sources[at_v] = wk, wv
    for j, c in enumerate(at_q):
        sources[c] = wq.at[:, pl.ds(j * kw, kw)]
    load_w = [
        pltpu.make_async_copy(source, item(c, z), load_sem.at[c])
        for c, source in enumerate(sources)
    ]
    load_o = pltpu.make_async_copy(wo, obuf.at[z], load_sem.at[nc])
    load_x = [
        pltpu.make_async_copy(hid_in, hid, load_sem.at[nc + 1]),
        pltpu.make_async_copy(ngain_in, ngain_t, load_sem.at[nc + 2]),
    ]
    load_r = [
        pltpu.make_async_copy(pgain_in, pgain_t, load_sem.at[nc + 3]),
        pltpu.make_async_copy(cos_in, cos_ref, load_sem.at[nc + 4]),
        pltpu.make_async_copy(sin_in, sin_ref, load_sem.at[nc + 5]),
        pltpu.make_async_copy(len_in, len_ref, load_sem.at[nc + 6]),
    ]
    for load in load_w[:1] + load_x + load_w[1:] + [load_o] + load_r:
        load.start()

    barrier = pltpu.get_barrier_semaphore()

    def greet(dp_index, mp_index):
        pl.semaphore_signal(barrier, inc=1, device_id=(dp_index, mp_index), device_id_type=MESH)

    greet(partner, mp)
    for step in range(1, n_mp):
        greet(me, lax.rem(mp + step, n_mp))

    @pl.when(can_up)
    def _():
        greet(me + 2, mp)

    @pl.when(can_down)
    def _():
        greet(me - 2, mp)

    pl.semaphore_wait(
        barrier, n_mp + jnp.where(can_up, 1, 0) + jnp.where(can_down, 1, 0)
    )

    def copy(c, origin, way):
        ref = item(c, origin)
        return remote(
            ref, ref, zsend.at[1 if c in lent else 0, way, origin], zrecv.at[c, origin],
            (me + 2, me - 2)[way], mp,
        )

    def sends(c, origin, way):
        if way == UP:
            skip, able = (z + 1 == nz - 1) & (origin < half), can_up
        else:
            skip, able = (z - 1 == 0) & (origin >= half), can_down
        return able & jnp.logical_not(skip) if c in lent else able

    def gets(c, origin):
        if c not in lent:
            return (origin >= 0) & (origin < nz)
        low, high = jnp.where(z == nz - 1, half, 0), jnp.where(z == 0, half, nz)
        return (origin >= low) & (origin < high)

    def send(c, origin, way):
        @pl.when(sends(c, origin, way))
        def _():
            copy(c, origin, way).start()

    def send_own(c):
        send(c, z, UP)
        send(c, z, DOWN)

    def send_own_out(c, down, up):
        @pl.when(down & middle)
        def _():
            copy(c, z, DOWN).start()

        @pl.when(up & middle)
        def _():
            copy(c, z, UP).start()

    def relay(c, k):
        for origin, way in ((z - k, UP), (z + k, DOWN)):
            @pl.when(gets(c, origin))
            def _():
                copy(c, origin, way).wait_recv()
                send(c, origin, way)

    def relays(c, first, last):
        def body(k, carry):
            relay(c, k)
            return carry

        lax.fori_loop(first, last, body, 0)

    def rows_of(parity, block):
        return pl.ds(pl.multiple_of(parity * maxlen + block * local_len, local_len), local_len)

    def region(parity, block):
        return nbuf.at[:, rows_of(parity, block), :]

    def across():
        return remote(
            nbuf.at[:, pl.ds(2 * maxlen, local_len), :], region(x, mp),
            xsend.at[0], xrecv.at[x, mp], partner, mp,
        )

    def to_mate(parity, block):
        return remote(
            region(parity, block), region(parity, block),
            xmate.at[parity, block // 2], xrecv.at[parity, block], me, mate,
        )

    def to_far(parity, step):
        return remote(
            region(parity, mp), region(parity, mp),
            xfar.at[parity, step - 1], xrecv.at[parity, mp], me, lax.rem(mp + 2 * step, n_mp),
        )

    def arrived(parity, block):
        return remote(
            region(parity, block), region(parity, block),
            xsend.at[0], xrecv.at[parity, block], me, mate,
        )

    def spread(parity):
        for step in range(1, pairs):
            to_far(parity, step).start()
        to_mate(parity, mp).start()

    def pass_on(parity):
        for step in range(1, pairs):
            block = lax.rem(mp + 2 * step, n_mp)
            arrived(parity, block).wait_recv()
            to_mate(parity, block).start()

    def lend(parity):
        return remote(
            nbuf.at[far_half, rows_of(parity, mp), :],
            hrows.at[rows_of(parity, mp), :],
            lsend.at[parity], lrecv.at[parity, mp], inward, mp,
        )

    def lent_to(parity, block, dst, send_sem):
        ref = hrows.at[rows_of(parity, block), :]
        return remote(ref, ref, send_sem, lrecv.at[parity, block], me, dst)

    def lent_mate(parity, block):
        return lent_to(parity, block, mate, lmate.at[parity, block // 2])

    def lent_far(parity, step):
        return lent_to(parity, mp, lax.rem(mp + 2 * step, n_mp), lfar.at[parity, step - 1])

    def lent_wait(parity, block):
        lent_to(parity, block, mate, lsend.at[parity]).wait_recv()

    def lent_spread(parity):
        lent_wait(parity, mp)
        for step in range(1, pairs):
            lent_far(parity, step).start()
        lent_mate(parity, mp).start()

    def lent_pass(parity):
        for step in range(1, pairs):
            block = lax.rem(mp + 2 * step, n_mp)
            lent_wait(parity, block)
            lent_mate(parity, block).start()

    load_w[0].wait()
    send_own(0)
    for load in load_x:
        load.wait()
    for t in range(width // LANES):
        ngain[:, t * LANES : (t + 1) * LANES] = ngain_t[t : t + 1, :]
    total = jnp.zeros((local_len, LANES), f32)
    for t in range(width // LANES):
        rows = hid[:, t * LANES : (t + 1) * LANES].astype(f32)
        total = total + rows * rows
    scale = lax.rsqrt(jnp.sum(total, axis=-1, keepdims=True) / width + 1e-06)
    for block in range(n_dp):
        span = slice(block * fcols, (block + 1) * fcols)
        rows = hid[:, span].astype(f32)
        first = jnp.where(x == block % 2, x * maxlen + mp * local_len, 2 * maxlen)
        k = block // 2
        cols = slice(k % half * fcols, (k % half + 1) * fcols)
        nbuf[k // half, pl.ds(pl.multiple_of(first, local_len), local_len), cols] = (
            rows * scale * ngain[:, span]
        ).astype(bf16)
    across().start()
    spread(x)

    @pl.when(ends)
    def _():
        lend(x).start()

    load_w[1].wait()
    send_own(1)
    acc[...] = jnp.zeros_like(acc)

    @pl.when(middle)
    def _():
        epin[...] = jnp.zeros_like(epin)

    def rollout_rows(parity):
        return pl.ds(pl.multiple_of(parity * maxlen, maxlen), maxlen)

    def swap(c):
        return remote(pout.at[c], pin.at[c], qsend.at[c], qrecv.at[c], partner, mp)

    def compute(c):
        first, last = 0, 2
        if c in lent:
            first, last = jnp.where(z == nz - 1, 1, 0), jnp.where(z == 0, 1, 2)

        def contract(parity):
            rows = rollout_rows(parity)

            def body(k, carry):
                acc[c, rows, :] += jnp.dot(
                    nbuf[k, rows, :], wbuf[c, k], preferred_element_type=f32
                )
                return carry

            lax.fori_loop(first, last, body, 0)

        contract(1 - x)
        pout[c] = acc[c, rollout_rows(1 - x), :].astype(bf16)
        swap(c).start()
        contract(x)

    def lent_swap(i):
        return remote(hpout.at[i], hpin.at[i], bsend.at[i], brecv.at[i], partner, mp)

    def lent_return(i):
        return remote(hsum.at[i], epin.at[i], esend.at[i], erecv.at[i], outward, mp)

    def lent_compute(i):
        def contract(parity):
            rows = rollout_rows(parity)

            hacc[i, rows, :] = jnp.dot(
                hrows[rows, :], wbuf[lent[i], far_half], preferred_element_type=f32
            )

        contract(1 - x)
        hpout[i] = hacc[i, rollout_rows(1 - x), :].astype(bf16)
        lent_swap(i).start()
        contract(x)

    def lent_finish(i):
        lent_swap(i).wait_recv()
        hsum[i] = (hacc[i, rollout_rows(x), :] + hpin[i].astype(f32)).astype(bf16)
        lent_return(i).start()

    def lent_add(i, cols):
        return epin[i, :, cols].astype(f32)

    def lent_ready(i):
        @pl.when(ends)
        def _():
            lent_return(i).wait_recv()

    def rotated(block, span):
        return block * cos_ref[span, :] + pltpu.roll(block, HD // 2, 1) * sin_ref[span, :]

    everything = slice(0, maxlen)

    def keys_done():
        swap(at_k).wait_recv()
        lent_ready(0)
        for h in range(kv_heads):
            cols = slice(h * HD, (h + 1) * HD)
            raw = acc[at_k, rollout_rows(x), cols] + pin[at_k, :, cols].astype(f32)
            raw = raw + lent_add(0, cols)
            kbuf[:, cols] = jnp.where(live, rotated(raw, everything), 0.0).astype(bf16)

    def values_done():
        swap(at_v).wait_recv()
        lent_ready(1)
        for h in range(kv_heads):
            cols = slice(h * HD, (h + 1) * HD)
            raw = acc[at_v, rollout_rows(x), cols] + pin[at_v, :, cols].astype(f32)
            raw = raw + lent_add(1, cols)
            value = jnp.where(live, raw, 0.0).astype(bf16)
            vbuf[:, cols] = value
            vext[h, :, :HD] = value
            vext[h, :, HD:] = jnp.where(live, 1.0, 0.0).astype(bf16)

    def share(j, parity):
        ref = att.at[parity, :, pl.ds(j * kw, kw)]
        return remote(ref, ref, asend.at[j], arecv.at[j], partner, mp)

    def attend(j):
        swap(at_q[j]).wait_recv()
        for i in range(kv_heads):
            h = j * kv_heads + i
            kv = h * kv_heads // q_heads
            cols, kcols = slice(i * HD, (i + 1) * HD), slice(kv * HD, (kv + 1) * HD)
            for r in range(n_mp):
                span, seen = slice(r * local_len, (r + 1) * local_len), (r + 1) * local_len
                raw = acc[at_q[j], rows_of(x, r), cols] + pin[at_q[j], span, cols].astype(f32)
                query = (rotated(raw, span) * 144.0 ** (-0.5)).astype(bf16)
                score = lax.dot_general(
                    query, kbuf[:seen, kcols], (((1,), (1,)), ((), ())),
                    preferred_element_type=f32,
                )
                row = lax.broadcasted_iota(jnp.int32, score.shape, 0) + r * local_len
                col = lax.broadcasted_iota(jnp.int32, score.shape, 1)
                expo = jnp.exp2(jnp.tanh(score * (1.0 / 50.0)) * (50.0 * np.log2(np.e)))
                expo = jnp.where(col <= row, expo, 0.0).astype(bf16)
                both = jnp.dot(expo, vext[kv, :seen, :], preferred_element_type=f32)
                att[x, span, h * HD : (h + 1) * HD] = (both[:, :HD] / both[:, HD:]).astype(bf16)
        share(j, x).start()

    relays(0, 1, 2)
    arrived(1 - x, mp).wait_recv()
    spread(1 - x)

    @pl.when(ends)
    def _():
        lend(1 - x).start()

    for load in load_w[2:] + [load_o]:
        load.wait()
    send_own(2)

    @pl.when(ends)
    def _():
        for c in range(3, nc + ns):
            send_own(c)

    pass_on(x)

    @pl.when(helps)
    def _():
        lent_spread(x)

    relays(0, 2, nz)
    relays(1, 1, 2)
    @pl.when(middle)
    def _():
        for c in range(3, nc):
            send_own(c)

    early = {0, ns - 1}
    for s in sorted(early):
        send_own_out(nc + s, z == 1, z == nz - 2)

    @pl.when(helps)
    def _():
        lent_spread(1 - x)

    pass_on(1 - x)
    for parity in (x, 1 - x):
        for step in range(pairs):
            arrived(parity, lax.rem(mate + 2 * step, n_mp)).wait_recv()
    compute(0)

    @pl.when(helps)
    def _():
        lent_pass(x)

    relays(1, 2, nz)
    relays(2, 1, 2)
    compute(1)

    @pl.when(helps)
    def _():
        lent_pass(1 - x)
        for parity in (x, 1 - x):
            for step in range(pairs):
                lent_wait(parity, lax.rem(mate + 2 * step, n_mp))
        lent_compute(0)

    for c in range(3, nc):
        relays(c, 1, 2)
    for load in load_r:
        load.wait()
    length = len_ref[0]
    live = lax.broadcasted_iota(jnp.int32, (maxlen, HD), 0) < length
    for t in range(width // LANES):
        pgain[:, t * LANES : (t + 1) * LANES] = pgain_t[t : t + 1, :]
    relays(2, 2, nz)

    @pl.when(helps)
    def _():
        lent_compute(1)

    compute(2)

    @pl.when(helps)
    def _():
        lent_finish(0)

    for c in range(3, nc):
        relays(c, 2, nz)
        compute(c)

    @pl.when(helps)
    def _():
        lent_finish(1)

    for s in range(ns):
        sent_out = s in early
        send_own_out(nc + s, z != 1 if sent_out else True, z != nz - 2 if sent_out else True)

    keys_done()
    values_done()
    for j in range(nq - 1):
        attend(j)

    def hand(s, zk, role, parity):
        return remote(
            psend[s].at[zk, parity, 1 - side], inbox[s].at[zk, parity],
            hsend.at[s], hrecv.at[s, zk, role], me, mate,
        )

    def far(s, zk, role, parity, step):
        target = lax.rem(mp + 2 * step, n_mp)
        return remote(
            psend[s].at[zk, parity, side, target // 2], precv[s].at[zk, parity, step - 1],
            fsend.at[s], frecv.at[s, zk, role, step - 1], me, target,
        )

    def back(s, zk, parity):
        return remote(
            xout[s].at[zk], yall[s].at[parity, zk], csend.at[s], crecv.at[s], partner, mp
        )

    def roles_of(s):
        return (OTHER,) if packed(pieces[s][1]) else (OTHER, OWN)

    def parity_of(role):
        return x if role == OWN else 1 - x

    def lead_of(s, role):
        return 0 if packed(pieces[s][1]) else parity_of(role)

    def produce(s, zk, role):
        start, size = pieces[s]
        lead = lead_of(s, role)

        def project(parity, weights):
            return lax.dot_general(
                att[parity], weights, (((1,), (1,)), ((), ())), preferred_element_type=f32
            )

        weights = obuf[zk, start : start + size, :]
        if packed(size):
            blank = jnp.zeros_like(weights)
            part = project(0, jnp.concatenate([weights, blank], axis=0))
            part = part + project(1, jnp.concatenate([blank, weights], axis=0))
        else:
            part = project(lead, weights)
        part = part.astype(bf16)
        for p in range(n_mp):
            psend[s][zk, lead, p % 2, p // 2] = part[p * local_len : (p + 1) * local_len]
        hand(s, zk, role, lead).start()

    def combine(s, zk, role):
        parity = lead_of(s, role)
        hand(s, zk, role, parity).wait_recv()
        for step in range(1, pairs):
            q = lax.rem(mp + 2 * step, n_mp) // 2
            both = psend[s][zk, parity, side, q].astype(f32) + inbox[s][zk, parity, q].astype(f32)
            psend[s][zk, parity, side, q] = both.astype(bf16)
            far(s, zk, role, parity, step).start()

    def measure(value):
        value = value.astype(f32)
        sq[...] += jnp.sum(value * value, axis=-1, keepdims=True)

    def settle(s, zk, role):
        parity = lead_of(s, role)
        value = psend[s][zk, parity, side, slot].astype(f32)
        value = value + inbox[s][zk, parity, slot].astype(f32)
        for step in range(1, pairs):
            far(s, zk, role, parity, step).wait_recv()
            value = value + precv[s][zk, parity, step - 1].astype(f32)
        size = pieces[s][1]
        if packed(size):
            swapped = pltpu.roll(value, size, 1)
            ours = jnp.where(x == 0, value, swapped)[:, :size].astype(bf16)
            theirs = jnp.where(x == 0, swapped, value)[:, :size].astype(bf16)
            xout[s][zk] = theirs
            back(s, zk, x).start()
            yall[s][x, zk] = ours
            measure(ours)
            return
        value = value.astype(bf16)
        if role == OWN:
            yall[s][x, zk] = value
            measure(value)
        else:
            xout[s][zk] = value
            back(s, zk, x).start()

    def around(k, act):
        def body(way, carry):
            zk = z + k * (2 * way - 1)

            @pl.when((zk >= 0) & (zk < nz) & ((way == 0) | (k > 0)))
            def _():
                act(zk)

            return carry

        lax.fori_loop(0, 2, body, 0)

    def near(act):
        def body(k, carry):
            around(k, act)
            return carry

        lax.fori_loop(0, min(2, nz), body, 0)

    attend(nq - 1)
    sq[...] = jnp.zeros_like(sq)
    single = [s for s in range(ns) if OWN in roles_of(s)]
    for s in single:
        produce(s, z, OWN)
    for s in range(ns):
        relays(nc + s, 1, 2)
        if s in single:
            combine(s, z, OWN)
    for s in single:
        around(1, functools.partial(produce, s, role=OWN))
    for s in single:
        around(1, functools.partial(combine, s, role=OWN))
    for j in range(nq):
        share(j, 1 - x).wait_recv()
    for s in range(ns):
        near(functools.partial(produce, s, role=OTHER))
        if s > 0:
            near(functools.partial(combine, s - 1, role=OTHER))
    near(functools.partial(combine, ns - 1, role=OTHER))

    def settle_near():
        for role in (OTHER, OWN):
            for s in range(ns):
                if role in roles_of(s):
                    late_here = True if role == OWN or s == ns - 1 else middle

                    @pl.when(late_here)
                    def _():
                        near(functools.partial(settle, s, role=role))

    def settle_at(s, k):
        def both(zk):
            for role in roles_of(s):
                settle(s, zk, role)

        around(k, both)

    def late(k, carry):
        for s in range(ns):
            relay(nc + s, k)

            def make(zk, s=s):
                for role in roles_of(s):
                    produce(s, zk, role)

            def join(zk, s=s):
                for role in roles_of(s):
                    combine(s, zk, role)

            around(k, make)
            around(k, join)
            if s == 0:
                @pl.when(k == 3)
                def _():
                    settle_near()
            else:
                @pl.when((k == 2) & ends)
                def _():
                    near(functools.partial(settle, s - 1, role=OTHER))

            @pl.when(k > 2)
            def _():
                settle_at(s, k - 1)

        return carry

    lax.fori_loop(2, nz, late, 0)
    if nz < 4:
        settle_near()
    if nz > 2:
        for s in range(ns):
            settle_at(s, nz - 1)

    for s in range(ns):
        remote(xout[s], yall[s].at[1 - x], csend.at[s], crecv.at[s], partner, mp).wait_recv()

    def collect(zk, carry):
        for s in range(ns):
            measure(yall[s][1 - x, zk])
        return carry

    lax.fori_loop(0, nz, collect, 0)

    scale = lax.rsqrt(sq[...] / width + 1e-06)
    for block in range(n_dp):
        for s, (start, size) in enumerate(pieces):
            span = slice(block * fcols + start, block * fcols + start + size)
            own = lax.broadcasted_iota(jnp.int32, (local_len, size), 0) + mp * local_len < length
            post = yall[s][block % 2, block // 2].astype(f32) * scale * pgain[:, span]
            mbuf[:, span] = jnp.where(own, hid[:, span].astype(f32) + post, 0.0).astype(bf16)

    def sent(ref, sem):
        remote(ref, ref, sem, sem, partner, mp).wait_send()

    def drain_items(origin, carry):
        for way, mine in ((UP, origin <= z), (DOWN, origin >= z)):
            @pl.when(mine & sends(nc, origin, way))
            def _():
                sent(obuf.at[pl.ds(0, 2)], zsend.at[0, way, origin])

            @pl.when(mine & sends(at_k, origin, way))
            def _():
                sent(wbuf.at[pl.ds(at_k, 2), 0, pl.ds(0, rows_each)], zsend.at[1, way, origin])

        return carry

    lax.fori_loop(0, nz, drain_items, 0)
    for s in range(ns):
        sent(psend[s].at[:, :, 0], hsend.at[s])
        if pairs > 1:
            sent(precv[s], fsend.at[s])
        sent(xout[s], csend.at[s])
    across().wait_send()
    for parity in (x, 1 - x):
        for step in range(1, pairs):
            to_far(parity, step).wait_send()
        for step in range(pairs):
            to_mate(parity, lax.rem(mp + 2 * step, n_mp)).wait_send()
    for c in range(nc):
        swap(c).wait_send()

    @pl.when(ends)
    def _():
        for parity in range(2):
            lend(parity).wait_send()

    @pl.when(helps)
    def _():
        for parity in (x, 1 - x):
            for step in range(1, pairs):
                lent_far(parity, step).wait_send()
            for step in range(pairs):
                lent_mate(parity, lax.rem(mp + 2 * step, n_mp)).wait_send()
        for i in range(len(lent)):
            lent_swap(i).wait_send()
            lent_return(i).wait_send()

    for j in range(nq):
        share(j, x).wait_send()


def local(n_dp, n_mp, hidden, lengths, norm_gain, w_query, w_key, w_value, w_out, post_gain):
    _, local_len, width = hidden.shape
    maxlen = local_len * n_mp
    rows, qw = w_query.shape
    kw = w_key.shape[1]
    orows, fcols = w_out.shape
    nz, pairs = n_dp // 2, n_mp // 2
    far = max(1, pairs - 1)
    nq = qw // kw
    nc = 2 + nq
    pieces = cut(fcols)
    ns = len(pieces)
    cosine, sine = tables(maxlen)
    anywhere = pl.BlockSpec(memory_space=pl.ANY)
    bf16, f32 = jnp.bfloat16, jnp.float32
    dma = pltpu.SemaphoreType.DMA
    tiles = (width // LANES, LANES)

    def per_piece(*lead):
        return [pltpu.VMEM((*lead, local_len, size), bf16) for _, size in pieces]

    def per_sum(*rest):
        return [
            pltpu.VMEM((nz, 1 if packed(size) else 2, *rest, local_len, size * (1 + packed(size))), bf16)
            for _, size in pieces
        ]

    mixed, keys, values = pl.pallas_call(
        functools.partial(kernel, n_dp, n_mp, pieces),
        out_shape=(
            pltpu.VMEM((local_len, width), bf16),
            pltpu.VMEM((maxlen, kw), bf16),
            pltpu.VMEM((maxlen, kw), bf16),
        ),
        in_specs=[anywhere] * 10,
        out_specs=(pl.BlockSpec(memory_space=pltpu.VMEM),) * 3,
        scratch_shapes=[
            pltpu.VMEM((local_len, width), bf16),
            pltpu.VMEM(tiles, f32),
            pltpu.VMEM(tiles, f32),
            pltpu.VMEM((1, width), f32),
            pltpu.VMEM((1, width), f32),
            pltpu.VMEM((maxlen, HD), f32),
            pltpu.VMEM((maxlen, HD), f32),
            pltpu.VMEM((nc, 2, nz // 2 * rows, kw), bf16),
            pltpu.VMEM((nz, fcols, orows), bf16),
            pltpu.VMEM((2, 2 * maxlen + local_len, nz // 2 * rows), bf16),
            pltpu.VMEM((nc, 2 * maxlen, kw), f32),
            pltpu.VMEM((nc, maxlen, kw), bf16),
            pltpu.VMEM((nc, maxlen, kw), bf16),
            pltpu.VMEM((kw // HD, maxlen, 2 * HD), bf16),
            pltpu.VMEM((2, maxlen, qw), bf16),
            pltpu.VMEM((local_len, 1), f32),
            pltpu.VMEM((2 * maxlen, nz // 2 * rows), bf16),
            pltpu.VMEM((2, 2 * maxlen, kw), f32),
            pltpu.VMEM((2, maxlen, kw), bf16),
            pltpu.VMEM((2, maxlen, kw), bf16),
            pltpu.VMEM((2, maxlen, kw), bf16),
            pltpu.VMEM((2, maxlen, kw), bf16),
            pltpu.SMEM((1,), jnp.int32),
            *per_sum(2, pairs),
            *per_sum(pairs),
            *per_sum(far),
            *per_piece(nz),
            *per_piece(2, nz),
            dma((nc + 7,)),
            dma((2, 2, nz)),
            dma((nc + ns, nz)),
            dma((1,)),
            dma((2, pairs)),
            dma((2, far)),
            dma((2, n_mp)),
            dma((nc,)),
            dma((nc,)),
            dma((nq,)),
            dma((nq,)),
            dma((ns,)),
            dma((ns, nz, 2)),
            dma((ns,)),
            dma((ns, nz, 2, far)),
            dma((ns,)),
            dma((ns,)),
            dma((2,)),
            dma((2, pairs)),
            dma((2, far)),
            dma((2, n_mp)),
            dma((2,)),
            dma((2,)),
            dma((2,)),
            dma((2,)),
        ],
        compiler_params=pltpu.CompilerParams(
            collective_id=0, has_side_effects=True, vmem_limit_bytes=60 * 1024 * 1024
        ),
    )(
        lengths,
        hidden[0],
        norm_gain.reshape(tiles),
        w_query,
        w_key,
        w_value,
        w_out.T,
        post_gain.reshape(tiles),
        jnp.asarray(cosine),
        jnp.asarray(sine),
    )
    return mixed[None], keys[None], values[None]


def solution(mesh):
    return jax.shard_map(
        functools.partial(local, mesh.shape["dp"], mesh.shape["mp"]),
        mesh=mesh,
        in_specs=(
            P("dp", "mp", None),
            P("dp"),
            P(),
            P("dp", "mp"),
            P("dp", "mp"),
            P("dp", "mp"),
            P("mp", "dp"),
            P(),
        ),
        out_specs=(P("dp", "mp", None), P("dp", None, "mp"), P("dp", None, "mp")),
        check_vma=False,
    )
```
